32 devices in a mesh: gx: 16 (over z, y, x), gy: 2 (over core).
Axes of the slice: x: 2, y: 2, z: 4, core: 2. Of those that a mesh axis runs over, the one named last changes fastest.
Arguments:
- bead_charge: float32 [16, 2, 16384], P('gx', 'gy'), may hold values from -6 to 6
- bead_cell: int32 [16, 2, 16384], P('gx', 'gy'), may hold values from 0 to 32767
- bead_count: int32 [16, 2], P('gx', 'gy'), may hold values from 8192 to 16384
- interp_weights: bfloat16 [16, 2, 12, 16384], P('gx', 'gy'), may hold values from 0.049804688 to 0.59765625
- kernel_fine: bfloat16 [17, 17, 17], replicated, may hold values from 0 to 4
- kernel_coarse: bfloat16 [17, 17, 17], replicated, may hold values from 0 to 4
Outputs:
- bead_potential: float32 [16, 2, 16384], P('gx', 'gy')
- potential_grid: float32 [256, 32, 128], P('gx', 'gy')
The draws below stay inside these ranges and needn't reach their ends.
All inputs are finite; a program needn't handle non-finite values.
Results may differ from the reference program's by a relative error of at most 0.00076.
Values may be sent and summed in bfloat16 or wider, within the bound.
No kernel may reach another device: no remote copies, remote signals or barrier semaphores. Data moves between devices by JAX's collectives and lax.ppermute only.
A program may use at most 64 MiB of HBM per device.

```python
import jax
import jax.numpy as jnp

LX = 16
LY = 16
LZ = 128
SLOTS = 16384
RADIUS = 8
NX = 256
NY = 32
NZ = 128
N_GX = 16
N_GY = 2


def kernel_shape(key, spread):
    side = 2 * RADIUS + 1
    offsets = jnp.arange(side, dtype=jnp.float32) - float(RADIUS)
    squared = offsets[:, None, None] * offsets[:, None, None] + offsets[None, :, None] * offsets[None, :, None] + offsets[None, None, :] * offsets[None, None, :]
    radius_cells = jnp.sqrt(squared)
    envelope = 1.0 / (1.0 + radius_cells / 6.0)
    jitter = jax.random.uniform(key, (side, side, side), jnp.float32, 1.0 - spread, 1.0 + spread)
    values = envelope * jitter
    return values * (4.0 / jnp.sqrt(jnp.sum(values * values)))


def draw_kernel_fine(key, part):
    values = kernel_shape(jax.random.fold_in(key, 11), 0.5)
    return values.astype(jnp.bfloat16)


def draw_kernel_coarse(key, part):
    values = kernel_shape(jax.random.fold_in(key, 23), 0.5)
    return values.astype(jnp.bfloat16)


def set_ends(array, stream_key, least, top_value):
    index_at = [jax.random.randint(jax.random.fold_in(stream_key, axis), (), 0, length) for axis, length in enumerate(array.shape)]
    main_axis = array.shape.index(max(array.shape))
    next_to = index_at[:main_axis] + [(index_at[main_axis] + 1) % array.shape[main_axis]] + index_at[main_axis + 1:]
    return array.at[tuple(index_at)].set(least).at[tuple(next_to)].set(top_value)


def steps_of(key, extent, split, smallest, high):
    gain, own = 1.0, jax.random.fold_in(key, 6)
    for axis_at, parts in split:
        heights = jnp.exp(jax.random.uniform(jax.random.fold_in(own, axis_at), (parts,), jnp.float32, smallest / len(split), high / len(split)))
        gain = gain * jnp.repeat(heights, extent[axis_at] // parts).reshape([-1 if axis == axis_at else 1 for axis in range(len(extent))])
    return gain


def gaussian(stream_key, dims, scale, bound, shards=(), kind=jnp.bfloat16):
    result = jax.random.normal(stream_key, dims, jnp.float32) * scale
    if len(shards) > 0:
        result = steps_of(stream_key, dims, shards, -0.22, 0.18) * result
    return jnp.clip(result, min=-bound, max=bound).astype(kind)


def setup_inputs(seed: int = 0) -> dict:
    key_list = jax.random.split(jax.random.key(seed), 7)
    return {
        "bead_charge": gaussian(key_list[0], (N_GX, N_GY, SLOTS), 1.0, 6.0, ((0, 16), (1, 2)), jnp.float32),
        "bead_cell": set_ends(jax.random.randint(key_list[1], (N_GX, N_GY, SLOTS), 0, LX * LY * LZ), jax.random.fold_in(key_list[1], 1), 0, (LX * LY * LZ) - 1).astype(jnp.int32),
        "bead_count": set_ends(jax.random.randint(key_list[2], (N_GX, N_GY), SLOTS // 2, SLOTS + 1), jax.random.fold_in(key_list[2], 1), SLOTS // 2, SLOTS).astype(jnp.int32),
        "interp_weights": jnp.clip(0.049804688 + 0.54785156 * jax.random.uniform(key_list[3], (N_GX, N_GY, 12, SLOTS), jnp.float32) ** steps_of(key_list[3], (N_GX, N_GY, 12, SLOTS), ((0, 16), (1, 2)), -0.2, 0.2), 0.049804688, 0.59765625).astype(jnp.bfloat16),
        "kernel_fine": draw_kernel_fine(jax.random.fold_in(key_list[6], 71), 0),
        "kernel_coarse": draw_kernel_coarse(jax.random.fold_in(key_list[6], 71), 0),
    }


SPLINE = (0.125, 0.5, 0.75, 0.5, 0.125)


def correlate(grid, kernel):
    shape_grid = grid.shape
    radius = (kernel.shape[0] - 1) // 2
    taps = jnp.arange(kernel.shape[0], dtype=jnp.int32) - radius
    index_first = ((-taps) % shape_grid[0])[:, None, None]
    index_second = ((-taps) % shape_grid[1])[None, :, None]
    index_third = ((-taps) % shape_grid[2])[None, None, :]
    table = jnp.zeros(shape_grid, grid.dtype)
    table = table.at[index_first, index_second, index_third].add(kernel.astype(grid.dtype))
    spectrum = jnp.fft.rfftn(grid) * jnp.fft.rfftn(table)
    return jnp.fft.irfftn(spectrum, s=shape_grid).astype(grid.dtype)


def restrict_grid(grid):
    for axis_number in range(3):
        summed = SPLINE[0] * jnp.roll(grid, 2, axis_number)
        for offset_one in range(1, 5):
            summed = summed + SPLINE[offset_one] * jnp.roll(grid, 2 - offset_one, axis_number)
        moved = jnp.moveaxis(summed, axis_number, 0)[::2]
        grid = jnp.moveaxis(moved, 0, axis_number)
    return grid


def refine_grid(grid):
    for axis_number in range(3):
        middle = jnp.moveaxis(grid, axis_number, 0)
        lower = jnp.roll(middle, 1, 0)
        upper = jnp.roll(middle, -1, 0)
        even_rows = (lower + 6.0 * middle + upper) * 0.125
        odd_rows = (middle + upper) * 0.5
        joined = jnp.stack([even_rows, odd_rows], axis=1).reshape((2 * middle.shape[0],) + middle.shape[1:])
        grid = jnp.moveaxis(joined, 0, axis_number)
    return grid


def reference(bead_charge, bead_cell, bead_count, interp_weights, kernel_fine, kernel_coarse):
    slot_index = jnp.arange(SLOTS, dtype=jnp.int32)
    live_slots = slot_index[None, None, :] < bead_count[:, :, None]
    values = jnp.where(live_slots, bead_charge, jnp.zeros_like(bead_charge))
    weights = interp_weights.astype(jnp.float32)
    brick_first = jnp.arange(N_GX, dtype=jnp.int32)[:, None, None]
    brick_second = jnp.arange(N_GY, dtype=jnp.int32)[None, :, None]
    cell_first = bead_cell // (LY * LZ) + brick_first * LX
    cell_second = (bead_cell // LZ) % LY + brick_second * LY
    cell_third = bead_cell % LZ
    charges = jnp.zeros((NX, NY, NZ), jnp.float32)
    for offset_one in range(4):
        for offset_two in range(4):
            for offset_three in range(4):
                contribution = values * weights[:, :, offset_one] * weights[:, :, 4 + offset_two] * weights[:, :, 8 + offset_three]
                charges = charges.at[(cell_first + offset_one) % NX, (cell_second + offset_two) % NY, (cell_third + offset_three) % NZ].add(contribution)
    fine_grid = charges.astype(jnp.bfloat16)
    fine_values = fine_grid.astype(jnp.float32)
    coarse_grid = restrict_grid(fine_values).astype(jnp.bfloat16)
    coarse_potential = correlate(coarse_grid.astype(jnp.float32), kernel_coarse.astype(jnp.float32))
    potential_grid = correlate(fine_values, kernel_fine.astype(jnp.float32)) + refine_grid(coarse_potential)
    bead_sum = jnp.zeros(values.shape, jnp.float32)
    for offset_one in range(4):
        for offset_two in range(4):
            for offset_three in range(4):
                factor = weights[:, :, offset_one] * weights[:, :, 4 + offset_two] * weights[:, :, 8 + offset_three]
                picked = potential_grid[(cell_first + offset_one) % NX, (cell_second + offset_two) % NY, (cell_third + offset_three) % NZ]
                bead_sum = bead_sum + factor * picked
    bead_potential = jnp.where(live_slots, bead_sum, jnp.zeros_like(bead_sum))
    return bead_potential, potential_grid
```

```python
import jax
import jax.numpy as jnp
from jax import lax
from jax.experimental import pallas as pl
from jax.experimental.pallas import tpu as pltpu
from jax.sharding import PartitionSpec as P

LX = 16
LY = 16
LZ = 128


SPLINE = (0.125, 0.5, 0.75, 0.5, 0.125)


def from_behind(value, axis, steps):
    count = lax.axis_size(axis)
    pairs = [(source, (source + steps) % count) for source in range(count)]
    return lax.ppermute(value, axis, pairs)


def extended_2(cells, sides, width):
    for axis, dim in sides:
        count = lax.axis_size(axis)
        head = lax.slice_in_dim(cells, 0, width, axis=dim)
        tail = lax.slice_in_dim(cells, cells.shape[dim] - width, cells.shape[dim], axis=dim)
        cells = jnp.concatenate(
            [
                lax.ppermute(tail, axis, [(i, (i + 1) % count) for i in range(count)]),
                cells,
                lax.ppermute(head, axis, [((i + 1) % count, i) for i in range(count)]),
            ],
            axis=dim,
        )
    return cells


def band_table(kernel_side, depth_cells):
    span_cells = depth_cells + kernel_side - 1
    shape_table = (kernel_side, span_cells, depth_cells)
    tap_index = lax.broadcasted_iota(jnp.int32, shape_table, 0)
    source = lax.broadcasted_iota(jnp.int32, shape_table, 1)
    target = lax.broadcasted_iota(jnp.int32, shape_table, 2)
    return (source - target == tap_index).astype(jnp.bfloat16)


def correlate(padded, kernel):
    kernel_side = kernel.shape[0]
    radius = (kernel_side - 1) // 2
    rows_first = padded.shape[0] - 2 * radius
    rows_second = padded.shape[1] - 2 * radius
    depth_cells = padded.shape[2]
    extended = jnp.concatenate(
        [padded[:, :, depth_cells - radius :], padded, padded[:, :, :radius]], axis=2
    )
    onehot = band_table(kernel_side, depth_cells)

    def add_plane(offset, summed):
        planes = lax.dynamic_slice_in_dim(extended, offset, rows_first, 0)
        window = jnp.stack(
            [planes[:, column : column + rows_second] for column in range(kernel_side)], axis=2
        )
        kernel_row = lax.dynamic_index_in_dim(kernel, offset, 0, keepdims=False)
        banded = jnp.einsum(
            "jk,kmc->jmc", kernel_row, onehot, preferred_element_type=jnp.float32
        ).astype(jnp.bfloat16)
        return summed + jnp.einsum(
            "abjm,jmc->abc", window, banded, preferred_element_type=jnp.float32
        )

    initial = jnp.zeros((rows_first, rows_second, depth_cells), jnp.float32)
    return lax.fori_loop(0, kernel_side, add_plane, initial)


def restrict_sides(padded, margin, count_first, count_second):
    values = padded.astype(jnp.float32)
    summed = SPLINE[0] * values[margin - 2 : margin - 2 + 2 * count_first : 2]
    for offset_one in range(1, 5):
        lowest = margin + offset_one - 2
        summed = summed + SPLINE[offset_one] * values[lowest : lowest + 2 * count_first : 2]
    values = summed
    summed = SPLINE[0] * values[:, margin - 2 : margin - 2 + 2 * count_second : 2]
    for offset_one in range(1, 5):
        lowest = margin + offset_one - 2
        summed = summed + SPLINE[offset_one] * values[:, lowest : lowest + 2 * count_second : 2]
    values = summed
    summed = SPLINE[0] * jnp.roll(values, 2, 2)
    for offset_one in range(1, 5):
        summed = summed + SPLINE[offset_one] * jnp.roll(values, 2 - offset_one, 2)
    return summed[:, :, ::2]


def refine_rows(values, count, leading):
    lower = values[leading - 1 : leading - 1 + count]
    middle = values[leading : leading + count]
    upper = values[leading + 1 : leading + 1 + count]
    even_rows = (lower + 6.0 * middle + upper) * 0.125
    odd_rows = (middle + upper) * 0.5
    return jnp.stack([even_rows, odd_rows], axis=1).reshape((2 * count,) + middle.shape[1:])


def refine_sides(padded, leading, count_first, count_second):
    along_first = refine_rows(padded, count_first, leading)
    moved = jnp.moveaxis(along_first, 1, 0)
    along_second = jnp.moveaxis(refine_rows(moved, count_second, leading), 0, 1)
    middle = jnp.moveaxis(along_second, 2, 0)
    lower = jnp.roll(middle, 1, 0)
    upper = jnp.roll(middle, -1, 0)
    even_rows = (lower + 6.0 * middle + upper) * 0.125
    odd_rows = (middle + upper) * 0.5
    joined = jnp.stack([even_rows, odd_rows], axis=1).reshape(
        (2 * middle.shape[0],) + middle.shape[1:]
    )
    return jnp.moveaxis(joined, 0, 2)


SPAN = 19
SPAN_PAD = 24
BLOCK = 512


def hat_rows(rows, start, weights, period):
    places = lax.broadcasted_iota(jnp.int32, (rows, start.shape[1]), 0) - start
    if period:
        places = places & (period - 1)
    table = jnp.where(places == 3, weights[3:4], 0.0)
    for offset in (2, 1, 0):
        table = jnp.where(places == offset, weights[offset : offset + 1], table)
    return table


def bead_tables(cells, weights):
    first = hat_rows(SPAN_PAD, cells // (LY * LZ), weights[0:4], 0)
    second = hat_rows(SPAN_PAD, cells // LZ % LY, weights[4:8], 0)
    depth = hat_rows(LZ, cells % LZ, weights[8:12], LZ)
    return first, second, depth


def spread_kernel(count_ref, charge_ref, cell_ref, weight_ref, out_ref):
    step = pl.program_id(0)

    @pl.when(step == 0)
    def _():
        out_ref[...] = jnp.zeros_like(out_ref)

    cells = cell_ref[0]
    weights = weight_ref[0, 0].astype(jnp.float32)
    first, second, depth = bead_tables(cells, weights)
    slots = lax.broadcasted_iota(jnp.int32, cells.shape, 1) + step * BLOCK
    amount = jnp.where(slots < count_ref[0, 0], charge_ref[0], 0.0)
    first = first * amount
    face = jnp.concatenate([first[row : row + 1] * second for row in range(SPAN)], axis=0)
    high = face.astype(jnp.bfloat16)
    low = (face - high.astype(jnp.float32)).astype(jnp.bfloat16)
    depth = depth.astype(jnp.bfloat16)
    dims = (((1,), (1,)), ((), ()))
    out_ref[...] += lax.dot_general(
        high, depth, dims, preferred_element_type=jnp.float32
    ) + lax.dot_general(low, depth, dims, preferred_element_type=jnp.float32)


def read_kernel(count_ref, grid_ref, cell_ref, weight_ref, out_ref):
    step = pl.program_id(0)
    cells = cell_ref[0]
    weights = weight_ref[0, 0].astype(jnp.float32)
    first, second, depth = bead_tables(cells, weights)
    depth = depth.astype(jnp.bfloat16)
    along = jnp.dot(
        grid_ref[...],
        jnp.concatenate([depth, depth], axis=0),
        preferred_element_type=jnp.float32,
    )
    total = first[0:1] * along[0:SPAN_PAD]
    for row in range(1, SPAN):
        total = total + first[row : row + 1] * along[row * SPAN_PAD : (row + 1) * SPAN_PAD]
    picked = jnp.sum(total * second, axis=0, keepdims=True)
    slots = lax.broadcasted_iota(jnp.int32, cells.shape, 1) + step * BLOCK
    out_ref[0] = jnp.where(slots < count_ref[0, 0], picked, 0.0)


def bead_specs():
    row = pl.BlockSpec((1, 1, BLOCK), lambda i: (0, 0, i))
    weight = pl.BlockSpec((1, 1, 12, BLOCK), lambda i: (0, 0, 0, i))
    return pl.BlockSpec(memory_space=pltpu.SMEM), row, weight


def spread_beads(count, charge, cell, weights):
    scalar, row, weight = bead_specs()
    return pl.pallas_call(
        spread_kernel,
        grid=(charge.shape[2] // BLOCK,),
        in_specs=[scalar, row, row, weight],
        out_specs=pl.BlockSpec((SPAN * SPAN_PAD, LZ), lambda i: (0, 0)),
        out_shape=jax.ShapeDtypeStruct((SPAN * SPAN_PAD, LZ), jnp.float32),
        name="spread",
    )(count, charge, cell, weights)


def read_beads(count, grid, cell, weights):
    scalar, row, weight = bead_specs()
    return pl.pallas_call(
        read_kernel,
        grid=(cell.shape[2] // BLOCK,),
        in_specs=[scalar, pl.BlockSpec(grid.shape, lambda i: (0, 0)), row, weight],
        out_specs=row,
        out_shape=jax.ShapeDtypeStruct(cell.shape, jnp.float32),
        name="read",
    )(count, grid, cell, weights)


def on_device(bead_charge, bead_cell, bead_count, interp_weights, kernel_fine, kernel_coarse):
    spread = spread_beads(bead_count, bead_charge, bead_cell, interp_weights)
    spread = spread.reshape(SPAN, SPAN_PAD, LZ)[:, :SPAN]
    from_below = from_behind(spread[LX:], "gx", 1)
    layered = spread[:LX].at[:3].add(from_below)
    from_side = from_behind(layered[:, LY:], "gy", 1)
    charges = layered[:, :LY].at[:, :3].add(from_side)
    fine_grid = charges.astype(jnp.bfloat16)
    radius = (kernel_fine.shape[0] - 1) // 2
    half_first = LX // 2
    half_second = LY // 2
    fine_padded = extended_2(fine_grid, (("gx", 0), ("gy", 1)), radius)
    coarse_grid = restrict_sides(fine_padded, radius, half_first, half_second).astype(jnp.bfloat16)
    coarse_padded = extended_2(coarse_grid, (("gx", 0), ("gy", 1)), radius)
    coarse_potential = correlate(coarse_padded, kernel_coarse)
    coarse_extended = extended_2(coarse_potential, (("gx", 0), ("gy", 1)), 3)
    fine_potential = correlate(fine_padded, kernel_fine)
    potential_grid = fine_potential + refine_sides(coarse_extended, 3, half_first, half_second)
    planes_above = from_behind(potential_grid[:3], "gx", -1)
    upward = jnp.concatenate([potential_grid, planes_above], axis=0)
    columns_above = from_behind(upward[:, :3], "gy", -1)
    potential_extended = jnp.concatenate(
        [upward, columns_above, jnp.zeros((SPAN, SPAN_PAD - SPAN, LZ), jnp.float32)], axis=1
    ).reshape(SPAN * SPAN_PAD, LZ)
    high = potential_extended.astype(jnp.bfloat16)
    low = (potential_extended - high.astype(jnp.float32)).astype(jnp.bfloat16)
    bead_potential = read_beads(
        bead_count, jnp.concatenate([high, low], axis=1), bead_cell, interp_weights
    )
    return (bead_potential, potential_grid)


def solution(mesh):
    return jax.shard_map(
        on_device,
        mesh=mesh,
        in_specs=(
            P("gx", "gy", None),
            P("gx", "gy", None),
            P("gx", "gy"),
            P("gx", "gy", None, None),
            P(),
            P(),
        ),
        out_specs=(P("gx", "gy", None), P("gx", "gy", None)),
        check_vma=False,
    )
```

```python
import jax
import jax.numpy as jnp
from jax import lax
from jax.experimental import pallas as pl
from jax.experimental.pallas import tpu as pltpu
from jax.sharding import PartitionSpec as P

LX = 16
LY = 16
LZ = 128
RADIUS = 8

SPAN = LX + 3
SPAN_PAD = 24
BLOCK = 512
REACH = 11
PLANES = SPAN + 2 * RADIUS
COLUMNS = 48
SHIFTS = RADIUS + 1
BANDS = 2 * RADIUS + 3
HALF = LZ // 2
KNOWN = 16
EDGE = 6
COARSE_OUT = 12
COARSE_IN = COARSE_OUT + 2 * RADIUS


def from_behind(value, axis, steps):
    count = lax.axis_size(axis)
    pairs = [(source, (source + steps) % count) for source in range(count)]
    return lax.ppermute(value, axis, pairs)


def hat_rows(rows, start, weights, period):
    places = lax.broadcasted_iota(jnp.int32, (rows, start.shape[1]), 0) - start
    if period:
        places = places & (period - 1)
    table = jnp.where(places == 3, weights[3:4], 0.0)
    for offset in (2, 1, 0):
        table = jnp.where(places == offset, weights[offset : offset + 1], table)
    return table


def bead_tables(cells, weights):
    first = hat_rows(SPAN_PAD, cells // (LY * LZ), weights[0:4], 0)
    second = hat_rows(SPAN_PAD, cells // LZ % LY, weights[4:8], 0)
    depth = hat_rows(LZ, cells % LZ, weights[8:12], LZ)
    return first, second, depth


def spread_kernel(count_ref, charge_ref, cell_ref, weight_ref, out_ref, up_ref, down_ref):
    step = pl.program_id(0)

    @pl.when(step == 0)
    def _():
        out_ref[...] = jnp.zeros_like(out_ref)

    cells = cell_ref[0]
    weights = weight_ref[0, 0].astype(jnp.float32)
    first, second, depth = bead_tables(cells, weights)
    slots = lax.broadcasted_iota(jnp.int32, cells.shape, 1) + step * BLOCK
    amount = jnp.where(slots < count_ref[0, 0], charge_ref[0], 0.0)
    first = first * amount
    face = jnp.concatenate([first[row : row + 1] * second for row in range(SPAN)], axis=0)
    high = face.astype(jnp.bfloat16)
    low = (face - high.astype(jnp.float32)).astype(jnp.bfloat16)
    depth = depth.astype(jnp.bfloat16)
    dims = (((1,), (1,)), ((), ()))
    out_ref[...] += lax.dot_general(
        high, depth, dims, preferred_element_type=jnp.float32
    ) + lax.dot_general(low, depth, dims, preferred_element_type=jnp.float32)

    @pl.when(step == pl.num_programs(0) - 1)
    def _():
        up_ref[...] = out_ref[(SPAN - REACH) * SPAN_PAD :].reshape(up_ref.shape)
        down_ref[...] = out_ref[: REACH * SPAN_PAD].reshape(down_ref.shape)


def read_kernel(count_ref, grid_ref, cell_ref, weight_ref, out_ref):
    step = pl.program_id(0)
    cells = cell_ref[0]
    weights = weight_ref[0, 0].astype(jnp.float32)
    first, second, depth = bead_tables(cells, weights)
    depth = depth.astype(jnp.bfloat16)
    along = jnp.dot(
        grid_ref[...],
        jnp.concatenate([depth, depth], axis=0),
        preferred_element_type=jnp.float32,
    )
    total = first[0:1] * along[0:SPAN_PAD]
    for row in range(1, SPAN):
        total = total + first[row : row + 1] * along[row * SPAN_PAD : (row + 1) * SPAN_PAD]
    picked = jnp.sum(total * second, axis=0, keepdims=True)
    slots = lax.broadcasted_iota(jnp.int32, cells.shape, 1) + step * BLOCK
    out_ref[0] = jnp.where(slots < count_ref[0, 0], picked, 0.0)


def bead_specs():
    row = pl.BlockSpec((1, 1, BLOCK), lambda i: (0, 0, i))
    weight = pl.BlockSpec((1, 1, 12, BLOCK), lambda i: (0, 0, 0, i))
    return pl.BlockSpec(memory_space=pltpu.SMEM), row, weight


def spread_beads(count, charge, cell, weights):
    scalar, row, weight = bead_specs()
    return pl.pallas_call(
        spread_kernel,
        grid=(charge.shape[2] // BLOCK,),
        in_specs=[scalar, row, row, weight],
        out_specs=(
            pl.BlockSpec((SPAN * SPAN_PAD, LZ), lambda i: (0, 0)),
            pl.BlockSpec((REACH, SPAN_PAD, LZ), lambda i: (0, 0, 0)),
            pl.BlockSpec((REACH, SPAN_PAD, LZ), lambda i: (0, 0, 0)),
        ),
        out_shape=(
            jax.ShapeDtypeStruct((SPAN * SPAN_PAD, LZ), jnp.float32),
            jax.ShapeDtypeStruct((REACH, SPAN_PAD, LZ), jnp.float32),
            jax.ShapeDtypeStruct((REACH, SPAN_PAD, LZ), jnp.float32),
        ),
        name="spread",
    )(count, charge, cell, weights)


def read_beads(count, grid, cell, weights):
    scalar, row, weight = bead_specs()
    return pl.pallas_call(
        read_kernel,
        grid=(cell.shape[2] // BLOCK,),
        in_specs=[scalar, pl.BlockSpec(grid.shape, lambda i: (0, 0)), row, weight],
        out_specs=row,
        out_shape=jax.ShapeDtypeStruct(cell.shape, jnp.float32),
        name="read",
    )(count, grid, cell, weights)


def spline_of(distance, period):
    place = (distance + 2) & (period - 1)
    return jnp.where(
        place == 2,
        0.75,
        jnp.where(
            (place == 1) | (place == 3), 0.5, jnp.where((place == 0) | (place == 4), 0.125, 0.0)
        ),
    )


def taps_on_lanes(kernel, depth, planes):
    kernel = kernel.astype(jnp.float32)
    side = kernel.shape[0]
    gap = jnp.zeros((side, side, depth - side), jnp.float32)
    lanes = jnp.concatenate([kernel[:, :, RADIUS::-1], gap, kernel[:, :, :RADIUS:-1]], axis=2)
    lanes = jnp.concatenate([lanes] * (LZ // depth), axis=2)
    return jnp.pad(lanes, ((0, planes - side), (1, SPAN_PAD - 1 - side), (0, 0)))


def circulant(row, rows):
    spread_out = jnp.broadcast_to(row, (rows, row.shape[1]))
    return pltpu.roll(spread_out, 0, 1, stride=1, stride_axis=0)


def fine_table_kernel(tap_ref, out_ref):
    for band in range(BANDS):
        out_ref[0, band] = circulant(tap_ref[0, band : band + 1], LZ).astype(jnp.bfloat16)


def fine_table(kernel):
    taps = taps_on_lanes(kernel, LZ, kernel.shape[0])
    return pl.pallas_call(
        fine_table_kernel,
        grid=(taps.shape[0],),
        in_specs=[pl.BlockSpec((1, SPAN_PAD, LZ), lambda i: (i, 0, 0))],
        out_specs=pl.BlockSpec((1, BANDS, LZ, LZ), lambda i: (i, 0, 0, 0)),
        out_shape=jax.ShapeDtypeStruct((taps.shape[0], BANDS, LZ, LZ), jnp.bfloat16),
        name="fine_table",
    )(taps)


def coarse_table_kernel(tap_ref, out_ref, band_ref):
    lower_half = lax.broadcasted_iota(jnp.int32, (HALF, LZ), 1) < HALF
    for side in range(2):
        for band in range(BANDS):
            band_ref[band] = circulant(tap_ref[side, band : band + 1], HALF)
        for shift in range(SHIFTS):
            for row in range(2):
                start = side * LZ + row * HALF
                out_ref[0, shift, start : start + HALF] = jnp.where(
                    lower_half, band_ref[2 * shift + 1 + row], band_ref[2 * shift + row]
                ).astype(jnp.bfloat16)


def coarse_table(kernel):
    pairs = (kernel.shape[0] + 1) // 2
    taps = taps_on_lanes(kernel, HALF, 2 * pairs)
    return pl.pallas_call(
        coarse_table_kernel,
        grid=(pairs,),
        in_specs=[pl.BlockSpec((2, SPAN_PAD, LZ), lambda i: (i, 0, 0))],
        out_specs=pl.BlockSpec((1, SHIFTS, 2 * LZ, LZ), lambda i: (i, 0, 0, 0)),
        out_shape=jax.ShapeDtypeStruct((pairs, SHIFTS, 2 * LZ, LZ), jnp.bfloat16),
        scratch_shapes=[pltpu.VMEM((BANDS, HALF, LZ), jnp.float32)],
        name="coarse_table",
    )(taps)


def three_terms(value):
    first = value.astype(jnp.bfloat16)
    rest = value - first.astype(jnp.float32)
    second = rest.astype(jnp.bfloat16)
    third = (rest - second.astype(jnp.float32)).astype(jnp.bfloat16)
    return first, second, third


def gather_kernel(own_ref, below_ref, above_ref, fine_ref, coarse_ref, half_ref):
    def put(first, last, value):
        fine_ref[:, first:last] = value.astype(jnp.bfloat16).astype(jnp.float32)

    put(0, 8, below_ref[:, 8:16])
    put(8, 16, own_ref[:, 0:8] + below_ref[:, 16:24])
    put(16, 24, own_ref[:, 8:16])
    put(24, 32, own_ref[:, 16:24] + above_ref[:, 0:8])
    put(32, 48, above_ref[:, 8:24])
    spline = (0.125, 0.5, 0.75, 0.5, 0.125)
    for plane in range(KNOWN):
        total = spline[0] * fine_ref[2 * plane]
        for step in range(1, 5):
            total = total + spline[step] * fine_ref[2 * plane + step]
        half_ref[plane] = total
    total = spline[0] * half_ref[:, pl.ds(0, KNOWN, stride=2)]
    for step in range(1, 5):
        total = total + spline[step] * half_ref[:, pl.ds(step, KNOWN, stride=2)]
    terms = jnp.concatenate(three_terms(total.reshape(KNOWN * KNOWN, LZ)), axis=1)
    shape = (3 * LZ, LZ)
    fine_depth = lax.broadcasted_iota(jnp.int32, shape, 0) & (LZ - 1)
    coarse_depth = lax.broadcasted_iota(jnp.int32, shape, 1) & (HALF - 1)
    table = spline_of(fine_depth - 2 * coarse_depth, LZ).astype(jnp.bfloat16)
    coarse = jnp.dot(terms, table, preferred_element_type=jnp.float32)
    coarse_ref[...] = coarse.astype(jnp.bfloat16).reshape(coarse_ref.shape)


def gather_fine(own, below, above):
    return pl.pallas_call(
        gather_kernel,
        out_shape=(
            jax.ShapeDtypeStruct((PLANES, COLUMNS, LZ), jnp.float32),
            jax.ShapeDtypeStruct((KNOWN, KNOWN, LZ), jnp.bfloat16),
        ),
        scratch_shapes=[pltpu.VMEM((KNOWN, COLUMNS, LZ), jnp.float32)],
        name="gather",
    )(own, below, above)


def fine_kernel(fine_ref, table_ref, out_ref, pair_ref):
    step = pl.program_id(0)

    @pl.when(step == 0)
    def _():
        out_ref[...] = jnp.zeros_like(out_ref)
        for shift in range(SHIFTS):
            halves = [fine_ref[:, pl.ds(2 * shift + part, 16, stride=2)] for part in range(2)]
            pair_ref[shift] = (
                jnp.concatenate(halves, axis=2).reshape(PLANES * 16, 2 * LZ).astype(jnp.bfloat16)
            )

    rows = pl.ds(pl.multiple_of(step * 16, 16), SPAN * 16)
    total = out_ref[...]
    for shift in range(SHIFTS):
        band = 2 * shift + 1
        upper = jnp.concatenate([table_ref[0, band], table_ref[0, band - 1]], axis=1)
        lower = jnp.concatenate([table_ref[0, band + 1], table_ref[0, band]], axis=1)
        total = total + jnp.dot(
            pair_ref[shift, rows],
            jnp.concatenate([upper, lower], axis=0),
            preferred_element_type=jnp.float32,
        )
    out_ref[...] = total


def fine_sums(fine, table):
    return pl.pallas_call(
        fine_kernel,
        grid=(table.shape[0],),
        in_specs=[
            pl.BlockSpec(fine.shape, lambda i: (0, 0, 0)),
            pl.BlockSpec((1, BANDS, LZ, LZ), lambda i: (i, 0, 0, 0)),
        ],
        out_specs=pl.BlockSpec((SPAN * 16, 2 * LZ), lambda i: (0, 0)),
        out_shape=jax.ShapeDtypeStruct((SPAN * 16, 2 * LZ), jnp.float32),
        scratch_shapes=[pltpu.VMEM((SHIFTS, PLANES * 16, 2 * LZ), jnp.bfloat16)],
        name="fine",
    )(fine, table)


def coarse_kernel(
    own_ref,
    below_ref,
    above_ref,
    low_ref,
    high_ref,
    table_ref,
    sums_ref,
    grid_ref,
    face_ref,
    cell_ref,
    pair_ref,
    total_ref,
    coarse_ref,
    wide_ref,
    join_ref,
):
    step = pl.program_id(0)

    @pl.when(step == 0)
    def _():
        total_ref[...] = jnp.zeros_like(total_ref)
        cell_ref[...] = jnp.zeros_like(cell_ref)
        for start, part in ((0, below_ref), (EDGE, own_ref), (EDGE + KNOWN, above_ref)):
            planes = slice(start, start + part.shape[0])
            values = part[...].astype(jnp.float32)
            cell_ref[planes, 8:24] = values
            if low_ref is None:
                cell_ref[planes, 0:8] = values[:, 8:16]
                cell_ref[planes, 24:32] = values[:, 0:8]
            else:
                cell_ref[planes, 0:8] = low_ref[planes].astype(jnp.float32)
                cell_ref[planes, 24:32] = high_ref[planes].astype(jnp.float32)
        lower_half = lax.broadcasted_iota(jnp.int32, (COARSE_IN + 1, 8, LZ), 2) < HALF
        for shift in range(SHIFTS):
            pair = jnp.where(
                lower_half,
                cell_ref[:, pl.ds(2 * shift + 2, 8, stride=2)],
                cell_ref[:, pl.ds(2 * shift + 3, 8, stride=2)],
            )
            rows = COARSE_IN * 8
            pair_ref[shift] = jnp.concatenate(
                [pair[:COARSE_IN].reshape(rows, LZ), pair[1:].reshape(rows, LZ)], axis=1
            ).astype(jnp.bfloat16)

    rows = pl.ds(pl.multiple_of(step * 16, 16), COARSE_OUT * 8)
    total = total_ref[...]
    for shift in range(SHIFTS):
        total = total + jnp.dot(
            pair_ref[shift, rows], table_ref[0, shift], preferred_element_type=jnp.float32
        )
    total_ref[...] = total

    @pl.when(step == pl.num_programs(0) - 1)
    def _():
        high = total.astype(jnp.bfloat16)
        low = (total - high.astype(jnp.float32)).astype(jnp.bfloat16)
        shape = (2 * LZ, 2 * LZ)
        source = lax.broadcasted_iota(jnp.int32, shape, 0)
        target = lax.broadcasted_iota(jnp.int32, shape, 1)
        table = jnp.where(
            (source // HALF) % 2 == target // LZ,
            spline_of((target & (LZ - 1)) - 2 * (source & (HALF - 1)), LZ),
            0.0,
        ).astype(jnp.bfloat16)
        deep = jnp.dot(
            jnp.concatenate([high, low], axis=1), table, preferred_element_type=jnp.float32
        )
        for part in range(2):
            coarse_ref[:, pl.ds(part, 8, stride=2)] = deep[:, part * LZ : (part + 1) * LZ].reshape(
                COARSE_OUT, 8, LZ
            )
        wide_ref[...] = jnp.zeros_like(wide_ref)
        for plane in range(SPAN):
            middle = plane // 2 + 1
            if plane % 2:
                value = (coarse_ref[middle] + coarse_ref[middle + 1]) * 0.5
            else:
                value = (
                    coarse_ref[middle - 1] + 6.0 * coarse_ref[middle] + coarse_ref[middle + 1]
                ) * 0.125
            wide_ref[plane, 0:16] = value
        before = wide_ref[:, 0:16]
        middle = wide_ref[:, 1:17]
        after = wide_ref[:, 2:18]
        even = (before + 6.0 * middle + after) * 0.125
        odd = (middle + after) * 0.5
        sums = sums_ref[...].reshape(SPAN, 16, 2 * LZ)
        join_ref[:, pl.ds(0, 16, stride=2)] = sums[:, :, :LZ] + even
        join_ref[:, pl.ds(1, 16, stride=2)] = sums[:, :, LZ:] + odd
        grid_ref[...] = join_ref[:LX, :LY]
        face = join_ref[:, :SPAN_PAD].reshape(SPAN * SPAN_PAD, LZ)
        face_high = face.astype(jnp.bfloat16)
        face_low = (face - face_high.astype(jnp.float32)).astype(jnp.bfloat16)
        face_ref[:, :LZ] = face_high
        face_ref[:, LZ:] = face_low


def potentials(own, below, above, low, high, table, sums):
    def whole(value):
        return pl.BlockSpec(value.shape, lambda i: (0,) * value.ndim)

    given = [own, below, above] + ([] if low is None else [low, high])
    specs = [whole(value) for value in given]
    specs.append(pl.BlockSpec((1, SHIFTS, 2 * LZ, LZ), lambda i: (i, 0, 0, 0)))
    specs.append(whole(sums))

    def body(*refs):
        if low is None:
            refs = refs[:3] + (None, None) + refs[3:]
        coarse_kernel(*refs)

    return pl.pallas_call(
        body,
        grid=(table.shape[0],),
        in_specs=specs,
        out_specs=(
            pl.BlockSpec((LX, LY, LZ), lambda i: (0, 0, 0)),
            pl.BlockSpec((SPAN * SPAN_PAD, 2 * LZ), lambda i: (0, 0)),
        ),
        out_shape=(
            jax.ShapeDtypeStruct((LX, LY, LZ), jnp.float32),
            jax.ShapeDtypeStruct((SPAN * SPAN_PAD, 2 * LZ), jnp.bfloat16),
        ),
        scratch_shapes=[
            pltpu.VMEM((COARSE_IN + 1, 40, LZ), jnp.float32),
            pltpu.VMEM((SHIFTS, COARSE_IN * 8, 2 * LZ), jnp.bfloat16),
            pltpu.VMEM((COARSE_OUT * 8, LZ), jnp.float32),
            pltpu.VMEM((COARSE_OUT, 16, LZ), jnp.float32),
            pltpu.VMEM((SPAN, 24, LZ), jnp.float32),
            pltpu.VMEM((SPAN, 32, LZ), jnp.float32),
        ],
        name="coarse",
    )(*given, table, sums)


def on_device(bead_charge, bead_cell, bead_count, interp_weights, kernel_fine, kernel_coarse):
    own, up, down = spread_beads(bead_count, bead_charge, bead_cell, interp_weights)
    below = from_behind(up, "gx", 1)
    above = from_behind(down, "gx", -1)
    table_fine = fine_table(kernel_fine)
    table_coarse = coarse_table(kernel_coarse)
    own = own.reshape(SPAN, SPAN_PAD, LZ)
    planes = jnp.concatenate(
        [
            below[:RADIUS],
            own[:3] + below[RADIUS:],
            own[3:LX],
            own[LX:] + above[:3],
            above[3:],
        ],
        axis=0,
    )
    wraps = lax.axis_size("gy") == 2
    columns_below = from_behind(planes, "gy", 1)
    columns_above = columns_below if wraps else from_behind(planes, "gy", -1)
    fine, coarse = gather_fine(planes, columns_below, columns_above)
    coarse_below = from_behind(coarse[2 : 2 + EDGE], "gx", 1)
    coarse_above = from_behind(coarse[8 : 8 + EDGE], "gx", -1)
    sums = fine_sums(fine, table_fine)
    low = high = None
    if not wraps:
        joined = jnp.concatenate([coarse_below, coarse, coarse_above], axis=0)
        low = from_behind(joined[:, :8], "gy", 1)
        high = from_behind(joined[:, 8:], "gy", -1)
    potential_grid, face = potentials(
        coarse, coarse_below, coarse_above, low, high, table_coarse, sums
    )
    bead_potential = read_beads(bead_count, face, bead_cell, interp_weights)
    return (bead_potential, potential_grid)


def solution(mesh):
    return jax.shard_map(
        on_device,
        mesh=mesh,
        in_specs=(
            P("gx", "gy", None),
            P("gx", "gy", None),
            P("gx", "gy"),
            P("gx", "gy", None, None),
            P(),
            P(),
        ),
        out_specs=(P("gx", "gy", None), P("gx", "gy", None)),
        check_vma=False,
    )
```

```python
import jax
import jax.numpy as jnp
from jax import lax
from jax.experimental import pallas as pl
from jax.experimental.pallas import tpu as pltpu
from jax.sharding import PartitionSpec as P

LX = 16
LY = 16
LZ = 128
RADIUS = 8

SPAN = LX + 3
SPAN_PAD = 24
BLOCK = 2048
VMEM_BYTES = 24 * 1024 * 1024
REACH = 11
PLANES = SPAN + 2 * RADIUS
COLUMNS = 48
SHIFTS = RADIUS + 1
BANDS = 2 * RADIUS + 3
HALF = LZ // 2
KNOWN = 16
EDGE = 6
COARSE_OUT = 12
COARSE_IN = COARSE_OUT + 2 * RADIUS


def from_behind(value, axis, steps):
    count = lax.axis_size(axis)
    pairs = [(source, (source + steps) % count) for source in range(count)]
    return lax.ppermute(value, axis, pairs)


def hat_rows(rows, start, weights, period):
    places = lax.broadcasted_iota(jnp.int32, (rows, start.shape[1]), 0) - start
    if period:
        places = places & (period - 1)
    table = jnp.where(places == 3, weights[3:4], 0.0)
    for offset in (2, 1, 0):
        table = jnp.where(places == offset, weights[offset : offset + 1], table)
    return table


def bead_tables(cells, weights):
    first = hat_rows(SPAN_PAD, cells // (LY * LZ), weights[0:4], 0)
    second = hat_rows(SPAN_PAD, cells // LZ % LY, weights[4:8], 0)
    depth = hat_rows(LZ, cells % LZ, weights[8:12], LZ)
    return first, second, depth


def spread_kernel(count_ref, charge_ref, cell_ref, weight_ref, out_ref, up_ref, down_ref):
    step = pl.program_id(0)

    @pl.when(step == 0)
    def _():
        out_ref[...] = jnp.zeros_like(out_ref)

    cells = cell_ref[0]
    weights = weight_ref[0, 0].astype(jnp.float32)
    first, second, depth = bead_tables(cells, weights)
    slots = lax.broadcasted_iota(jnp.int32, cells.shape, 1) + step * BLOCK
    amount = jnp.where(slots < count_ref[0, 0], charge_ref[0], 0.0)
    first = first * amount
    face = jnp.concatenate([first[row : row + 1] * second for row in range(SPAN)], axis=0)
    high = face.astype(jnp.bfloat16)
    low = (face - high.astype(jnp.float32)).astype(jnp.bfloat16)
    depth = depth.astype(jnp.bfloat16)
    dims = (((1,), (1,)), ((), ()))
    out_ref[...] += lax.dot_general(
        high, depth, dims, preferred_element_type=jnp.float32
    ) + lax.dot_general(low, depth, dims, preferred_element_type=jnp.float32)

    @pl.when(step == pl.num_programs(0) - 1)
    def _():
        up_ref[...] = out_ref[(SPAN - REACH) * SPAN_PAD :].reshape(up_ref.shape)
        down_ref[...] = out_ref[: REACH * SPAN_PAD].reshape(down_ref.shape)


def read_kernel(count_ref, grid_ref, cell_ref, weight_ref, out_ref):
    step = pl.program_id(0)
    cells = cell_ref[0]
    weights = weight_ref[0, 0].astype(jnp.float32)
    first, second, depth = bead_tables(cells, weights)
    depth = depth.astype(jnp.bfloat16)
    along = jnp.dot(
        grid_ref[...],
        jnp.concatenate([depth, depth], axis=0),
        preferred_element_type=jnp.float32,
    )
    total = first[0:1] * along[0:SPAN_PAD]
    for row in range(1, SPAN):
        total = total + first[row : row + 1] * along[row * SPAN_PAD : (row + 1) * SPAN_PAD]
    picked = jnp.sum(total * second, axis=0, keepdims=True)
    slots = lax.broadcasted_iota(jnp.int32, cells.shape, 1) + step * BLOCK
    out_ref[0] = jnp.where(slots < count_ref[0, 0], picked, 0.0)


def bead_specs():
    row = pl.BlockSpec((1, 1, BLOCK), lambda i: (0, 0, i))
    weight = pl.BlockSpec((1, 1, 12, BLOCK), lambda i: (0, 0, 0, i))
    return pl.BlockSpec(memory_space=pltpu.SMEM), row, weight


def spread_beads(count, charge, cell, weights):
    scalar, row, weight = bead_specs()
    return pl.pallas_call(
        spread_kernel,
        grid=(charge.shape[2] // BLOCK,),
        in_specs=[scalar, row, row, weight],
        out_specs=(
            pl.BlockSpec((SPAN * SPAN_PAD, LZ), lambda i: (0, 0)),
            pl.BlockSpec((REACH, SPAN_PAD, LZ), lambda i: (0, 0, 0)),
            pl.BlockSpec((REACH, SPAN_PAD, LZ), lambda i: (0, 0, 0)),
        ),
        out_shape=(
            jax.ShapeDtypeStruct((SPAN * SPAN_PAD, LZ), jnp.float32),
            jax.ShapeDtypeStruct((REACH, SPAN_PAD, LZ), jnp.float32),
            jax.ShapeDtypeStruct((REACH, SPAN_PAD, LZ), jnp.float32),
        ),
        name="spread",
        compiler_params=pltpu.CompilerParams(vmem_limit_bytes=VMEM_BYTES),
    )(count, charge, cell, weights)


def read_beads(count, grid, cell, weights):
    scalar, row, weight = bead_specs()
    return pl.pallas_call(
        read_kernel,
        grid=(cell.shape[2] // BLOCK,),
        in_specs=[scalar, pl.BlockSpec(grid.shape, lambda i: (0, 0)), row, weight],
        out_specs=row,
        out_shape=jax.ShapeDtypeStruct(cell.shape, jnp.float32),
        name="read",
        compiler_params=pltpu.CompilerParams(vmem_limit_bytes=VMEM_BYTES),
    )(count, grid, cell, weights)


def spline_of(distance, period):
    place = (distance + 2) & (period - 1)
    return jnp.where(
        place == 2,
        0.75,
        jnp.where(
            (place == 1) | (place == 3), 0.5, jnp.where((place == 0) | (place == 4), 0.125, 0.0)
        ),
    )


PERIOD = 32


def tap_rows(taps):
    side = taps.shape[0]
    tap = lax.broadcasted_iota(jnp.int32, (side, LZ), 0)
    lane = lax.broadcasted_iota(jnp.int32, (side, LZ), 1)
    table = jnp.where(((lane + tap - RADIUS) & (PERIOD - 1)) == 0, 1.0, 0.0).astype(jnp.bfloat16)
    return jnp.dot(taps, table, preferred_element_type=jnp.float32)


def turned(row):
    return pltpu.roll(
        jnp.broadcast_to(row, (PERIOD, row.shape[1])), 0, 1, stride=1, stride_axis=0
    )


def near_mask(rows, depth):
    row = lax.broadcasted_iota(jnp.int32, (rows, LZ), 0)
    lane = lax.broadcasted_iota(jnp.int32, (rows, LZ), 1)
    near = ((row - lane + RADIUS) & (depth - 1)) <= 2 * RADIUS
    return jnp.where(near, 1.0, 0.0).astype(jnp.bfloat16)


def coarse_table_kernel(tap_ref, out_ref, row_ref):
    step = pl.program_id(0)
    lower_half = lax.broadcasted_iota(jnp.int32, (PERIOD, LZ), 1) < HALF
    mask = near_mask(HALF, HALF)
    row_ref[...] = jnp.zeros_like(row_ref)
    last = tap_ref.shape[0] - 1
    for side in range(2):
        plane = jnp.minimum(2 * step + side, last)
        weight = jnp.where(2 * step + side <= last, 1.0, 0.0)
        row_ref[1 : 2 + last] = tap_rows(tap_ref[plane]) * weight
        before = turned(row_ref[0:1])
        for band in range(BANDS - 1):
            after = turned(row_ref[band + 1 : band + 2])
            block = jnp.where(lower_half, after, before).astype(jnp.bfloat16)
            start = side * LZ + (band % 2) * HALF
            out_ref[0, band // 2, start : start + HALF] = (
                jnp.concatenate([block] * (HALF // PERIOD), axis=0) * mask
            )
            before = after


def coarse_table(kernel):
    pairs = (kernel.shape[0] + 1) // 2
    return pl.pallas_call(
        coarse_table_kernel,
        grid=(pairs,),
        in_specs=[pl.BlockSpec(kernel.shape, lambda i: (0, 0, 0))],
        out_specs=pl.BlockSpec((1, SHIFTS, 2 * LZ, LZ), lambda i: (i, 0, 0, 0)),
        out_shape=jax.ShapeDtypeStruct((pairs, SHIFTS, 2 * LZ, LZ), jnp.bfloat16),
        scratch_shapes=[pltpu.VMEM((SPAN_PAD, LZ), jnp.float32)],
        name="coarse_table",
        compiler_params=pltpu.CompilerParams(vmem_limit_bytes=VMEM_BYTES),
    )(kernel)


def three_terms(value):
    first = value.astype(jnp.bfloat16)
    rest = value - first.astype(jnp.float32)
    second = rest.astype(jnp.bfloat16)
    third = (rest - second.astype(jnp.float32)).astype(jnp.bfloat16)
    return first, second, third


def merged_plane(pieces, plane):
    own, below, above = pieces
    inner = plane - RADIUS
    if inner < 0:
        return below[plane]
    value = own[inner * SPAN_PAD : (inner + 1) * SPAN_PAD] if inner < SPAN else None
    if plane < REACH:
        return value + below[plane]
    if inner < LX:
        return value
    outer = above[inner - LX]
    return outer if value is None else value + outer


def gather_kernel(*refs):
    fine_ref, coarse_ref, up_ref, down_ref, half_ref = refs[-5:]
    own, before = refs[0:3], refs[3:6]
    after = before if len(refs) == 11 else refs[6:9]
    for plane in range(PLANES):
        middle = merged_plane(own, plane)
        lower = merged_plane(before, plane)
        upper = merged_plane(after, plane)
        value = jnp.concatenate(
            [
                lower[8:16],
                middle[0:8] + lower[16:24],
                middle[8:16],
                middle[16:24] + upper[0:8],
                upper[8:24],
            ],
            axis=0,
        )
        fine_ref[plane] = value.astype(jnp.bfloat16).astype(jnp.float32)
    spline = (0.125, 0.5, 0.75, 0.5, 0.125)
    for plane in range(KNOWN):
        total = spline[0] * fine_ref[2 * plane]
        for step in range(1, 5):
            total = total + spline[step] * fine_ref[2 * plane + step]
        half_ref[plane] = total
    total = spline[0] * half_ref[:, pl.ds(0, KNOWN, stride=2)]
    for step in range(1, 5):
        total = total + spline[step] * half_ref[:, pl.ds(step, KNOWN, stride=2)]
    terms = jnp.concatenate(three_terms(total.reshape(KNOWN * KNOWN, LZ)), axis=1)
    shape = (3 * LZ, LZ)
    fine_depth = lax.broadcasted_iota(jnp.int32, shape, 0) & (LZ - 1)
    coarse_depth = lax.broadcasted_iota(jnp.int32, shape, 1) & (HALF - 1)
    table = spline_of(fine_depth - 2 * coarse_depth, LZ).astype(jnp.bfloat16)
    coarse = jnp.dot(terms, table, preferred_element_type=jnp.float32)
    coarse = coarse.astype(jnp.bfloat16).reshape(coarse_ref.shape)
    coarse_ref[...] = coarse
    up_ref[...] = coarse[2 : 2 + EDGE]
    down_ref[...] = coarse[8 : 8 + EDGE]


def gather_fine(pieces):
    edge = jax.ShapeDtypeStruct((EDGE, KNOWN, LZ), jnp.bfloat16)
    return pl.pallas_call(
        gather_kernel,
        out_shape=(
            jax.ShapeDtypeStruct((PLANES, COLUMNS, LZ), jnp.float32),
            jax.ShapeDtypeStruct((KNOWN, KNOWN, LZ), jnp.bfloat16),
            edge,
            edge,
        ),
        scratch_shapes=[pltpu.VMEM((KNOWN, COLUMNS, LZ), jnp.float32)],
        name="gather",
        compiler_params=pltpu.CompilerParams(vmem_limit_bytes=VMEM_BYTES),
    )(*pieces)


def fine_kernel(fine_ref, tap_ref, out_ref, pair_ref, row_ref, even_ref, odd_ref):
    side = tap_ref.shape[0]
    row_ref[...] = jnp.zeros_like(row_ref)
    for plane in range(side):
        row_ref[plane, 1 : 1 + side] = tap_rows(tap_ref[plane])
    for shift in range(SHIFTS):
        halves = [fine_ref[:, pl.ds(2 * shift + part, 16, stride=2)] for part in range(2)]
        pair_ref[shift] = (
            jnp.concatenate(halves, axis=2).reshape(PLANES * 16, 2 * LZ).astype(jnp.bfloat16)
        )
    out_ref[...] = jnp.zeros_like(out_ref)

    def build(table_ref, plane):
        mask = near_mask(LZ, LZ)
        for band in range(BANDS):
            block = turned(row_ref[plane, band : band + 1]).astype(jnp.bfloat16)
            table_ref[band] = jnp.concatenate([block] * (LZ // PERIOD), axis=0) * mask

    def multiply(table_ref, plane):
        rows = pl.ds(pl.multiple_of(plane * 16, 16), SPAN * 16)
        total = out_ref[...]
        for shift in range(SHIFTS):
            band = 2 * shift + 1
            upper = jnp.concatenate([table_ref[band], table_ref[band - 1]], axis=1)
            lower = jnp.concatenate([table_ref[band + 1], table_ref[band]], axis=1)
            total = total + jnp.dot(
                pair_ref[shift, rows],
                jnp.concatenate([upper, lower], axis=0),
                preferred_element_type=jnp.float32,
            )
        out_ref[...] = total

    build(even_ref, 0)

    def two_planes(index, carry):
        plane = 2 * index
        build(odd_ref, plane + 1)
        multiply(even_ref, plane)
        build(even_ref, plane + 2)
        multiply(odd_ref, plane + 1)
        return carry

    lax.fori_loop(0, side // 2, two_planes, 0)
    multiply(even_ref, side - 1)


def fine_sums(fine, kernel):
    return pl.pallas_call(
        fine_kernel,
        out_shape=jax.ShapeDtypeStruct((SPAN * 16, 2 * LZ), jnp.float32),
        scratch_shapes=[
            pltpu.VMEM((SHIFTS, PLANES * 16, 2 * LZ), jnp.bfloat16),
            pltpu.VMEM((kernel.shape[0], SPAN_PAD, LZ), jnp.float32),
            pltpu.VMEM((BANDS, LZ, LZ), jnp.bfloat16),
            pltpu.VMEM((BANDS, LZ, LZ), jnp.bfloat16),
        ],
        name="fine",
        compiler_params=pltpu.CompilerParams(vmem_limit_bytes=VMEM_BYTES),
    )(fine, kernel)


def coarse_kernel(
    own_ref,
    below_ref,
    above_ref,
    low_ref,
    high_ref,
    table_ref,
    sums_ref,
    grid_ref,
    face_ref,
    cell_ref,
    pair_ref,
    total_ref,
    coarse_ref,
    wide_ref,
    join_ref,
):
    step = pl.program_id(0)

    @pl.when(step == 0)
    def _():
        total_ref[...] = jnp.zeros_like(total_ref)
        cell_ref[...] = jnp.zeros_like(cell_ref)
        for start, part in ((0, below_ref), (EDGE, own_ref), (EDGE + KNOWN, above_ref)):
            planes = slice(start, start + part.shape[0])
            values = part[...].astype(jnp.float32)
            cell_ref[planes, 8:24] = values
            if low_ref is None:
                cell_ref[planes, 0:8] = values[:, 8:16]
                cell_ref[planes, 24:32] = values[:, 0:8]
            else:
                cell_ref[planes, 0:8] = low_ref[planes].astype(jnp.float32)
                cell_ref[planes, 24:32] = high_ref[planes].astype(jnp.float32)
        lower_half = lax.broadcasted_iota(jnp.int32, (COARSE_IN + 1, 8, LZ), 2) < HALF
        for shift in range(SHIFTS):
            pair = jnp.where(
                lower_half,
                cell_ref[:, pl.ds(2 * shift + 2, 8, stride=2)],
                cell_ref[:, pl.ds(2 * shift + 3, 8, stride=2)],
            )
            rows = COARSE_IN * 8
            pair_ref[shift] = jnp.concatenate(
                [pair[:COARSE_IN].reshape(rows, LZ), pair[1:].reshape(rows, LZ)], axis=1
            ).astype(jnp.bfloat16)

    rows = pl.ds(pl.multiple_of(step * 16, 16), COARSE_OUT * 8)
    total = total_ref[...]
    for shift in range(SHIFTS):
        total = total + jnp.dot(
            pair_ref[shift, rows], table_ref[0, shift], preferred_element_type=jnp.float32
        )
    total_ref[...] = total

    @pl.when(step == pl.num_programs(0) - 1)
    def _():
        high = total.astype(jnp.bfloat16)
        low = (total - high.astype(jnp.float32)).astype(jnp.bfloat16)
        shape = (2 * LZ, 2 * LZ)
        source = lax.broadcasted_iota(jnp.int32, shape, 0)
        target = lax.broadcasted_iota(jnp.int32, shape, 1)
        table = jnp.where(
            (source // HALF) % 2 == target // LZ,
            spline_of((target & (LZ - 1)) - 2 * (source & (HALF - 1)), LZ),
            0.0,
        ).astype(jnp.bfloat16)
        deep = jnp.dot(
            jnp.concatenate([high, low], axis=1), table, preferred_element_type=jnp.float32
        )
        for part in range(2):
            coarse_ref[:, pl.ds(part, 8, stride=2)] = deep[:, part * LZ : (part + 1) * LZ].reshape(
                COARSE_OUT, 8, LZ
            )
        wide_ref[...] = jnp.zeros_like(wide_ref)
        for plane in range(SPAN):
            middle = plane // 2 + 1
            if plane % 2:
                value = (coarse_ref[middle] + coarse_ref[middle + 1]) * 0.5
            else:
                value = (
                    coarse_ref[middle - 1] + 6.0 * coarse_ref[middle] + coarse_ref[middle + 1]
                ) * 0.125
            wide_ref[plane, 0:16] = value
        before = wide_ref[:, 0:16]
        middle = wide_ref[:, 1:17]
        after = wide_ref[:, 2:18]
        even = (before + 6.0 * middle + after) * 0.125
        odd = (middle + after) * 0.5
        sums = sums_ref[...].reshape(SPAN, 16, 2 * LZ)
        join_ref[:, pl.ds(0, 16, stride=2)] = sums[:, :, :LZ] + even
        join_ref[:, pl.ds(1, 16, stride=2)] = sums[:, :, LZ:] + odd
        grid_ref[...] = join_ref[:LX, :LY]
        face = join_ref[:, :SPAN_PAD].reshape(SPAN * SPAN_PAD, LZ)
        face_high = face.astype(jnp.bfloat16)
        face_low = (face - face_high.astype(jnp.float32)).astype(jnp.bfloat16)
        face_ref[:, :LZ] = face_high
        face_ref[:, LZ:] = face_low


def potentials(own, below, above, low, high, table, sums):
    def whole(value):
        return pl.BlockSpec(value.shape, lambda i: (0,) * value.ndim)

    given = [own, below, above] + ([] if low is None else [low, high])
    specs = [whole(value) for value in given]
    specs.append(pl.BlockSpec((1, SHIFTS, 2 * LZ, LZ), lambda i: (i, 0, 0, 0)))
    specs.append(whole(sums))

    def body(*refs):
        if low is None:
            refs = refs[:3] + (None, None) + refs[3:]
        coarse_kernel(*refs)

    return pl.pallas_call(
        body,
        grid=(table.shape[0],),
        in_specs=specs,
        out_specs=(
            pl.BlockSpec((LX, LY, LZ), lambda i: (0, 0, 0)),
            pl.BlockSpec((SPAN * SPAN_PAD, 2 * LZ), lambda i: (0, 0)),
        ),
        out_shape=(
            jax.ShapeDtypeStruct((LX, LY, LZ), jnp.float32),
            jax.ShapeDtypeStruct((SPAN * SPAN_PAD, 2 * LZ), jnp.bfloat16),
        ),
        scratch_shapes=[
            pltpu.VMEM((COARSE_IN + 1, 40, LZ), jnp.float32),
            pltpu.VMEM((SHIFTS, COARSE_IN * 8, 2 * LZ), jnp.bfloat16),
            pltpu.VMEM((COARSE_OUT * 8, LZ), jnp.float32),
            pltpu.VMEM((COARSE_OUT, 16, LZ), jnp.float32),
            pltpu.VMEM((SPAN, 24, LZ), jnp.float32),
            pltpu.VMEM((SPAN, 32, LZ), jnp.float32),
        ],
        name="coarse",
        compiler_params=pltpu.CompilerParams(vmem_limit_bytes=VMEM_BYTES),
    )(*given, table, sums)


def on_device(bead_charge, bead_cell, bead_count, interp_weights, kernel_fine, kernel_coarse):
    own, up, down = spread_beads(bead_count, bead_charge, bead_cell, interp_weights)
    below = from_behind(up, "gx", 1)
    above = from_behind(down, "gx", -1)
    table_coarse = coarse_table(kernel_coarse)
    wraps = lax.axis_size("gy") == 2
    pieces = [own, below, above]
    for steps in (1,) if wraps else (1, -1):
        pieces += [from_behind(part, "gy", steps) for part in (own, below, above)]
    fine, coarse, coarse_up, coarse_down = gather_fine(pieces)
    coarse_below = from_behind(coarse_up, "gx", 1)
    coarse_above = from_behind(coarse_down, "gx", -1)
    sums = fine_sums(fine, kernel_fine)
    low = high = None
    if not wraps:
        joined = jnp.concatenate([coarse_below, coarse, coarse_above], axis=0)
        low = from_behind(joined[:, :8], "gy", 1)
        high = from_behind(joined[:, 8:], "gy", -1)
    potential_grid, face = potentials(
        coarse, coarse_below, coarse_above, low, high, table_coarse, sums
    )
    bead_potential = read_beads(bead_count, face, bead_cell, interp_weights)
    return (bead_potential, potential_grid)


def solution(mesh):
    return jax.shard_map(
        on_device,
        mesh=mesh,
        in_specs=(
            P("gx", "gy", None),
            P("gx", "gy", None),
            P("gx", "gy"),
            P("gx", "gy", None, None),
            P(),
            P(),
        ),
        out_specs=(P("gx", "gy", None), P("gx", "gy", None)),
        check_vma=False,
    )
```

```python
import jax
import jax.numpy as jnp
from jax import lax
from jax.experimental import pallas as pl
from jax.experimental.pallas import tpu as pltpu
from jax.sharding import PartitionSpec as P

LX = 16
LY = 16
LZ = 128
RADIUS = 8

SPAN = LX + 3
SPAN_PAD = 24
BLOCK = 2048
CHUNK = 256
READ_CHUNK = 512
FACE = SPAN * LY + (SPAN - LY) * SPAN_PAD
VMEM_BYTES = 24 * 1024 * 1024
REACH = 11
PLANES = SPAN + 2 * RADIUS
COLUMNS = 48
SHIFTS = RADIUS + 1
BANDS = 2 * RADIUS + 3
HALF = LZ // 2
KNOWN = 16
EDGE = 6
COARSE_OUT = 12
COARSE_IN = COARSE_OUT + 2 * RADIUS


def from_behind(value, axis, steps):
    count = lax.axis_size(axis)
    pairs = [(source, (source + steps) % count) for source in range(count)]
    return lax.ppermute(value, axis, pairs)


def hat_rows(rows, start, weights, period):
    places = lax.broadcasted_iota(jnp.int32, (rows, start.shape[1]), 0) - start
    if period:
        places = places & (period - 1)
    table = jnp.where(places == 3, weights[3:4], 0.0)
    for offset in (2, 1, 0):
        table = jnp.where(places == offset, weights[offset : offset + 1], table)
    return table


def depth_rows(start, weights):
    groups = LZ // 8
    pattern = hat_rows(16, start & 7, weights, 0)
    low, high = pattern[:8], pattern[8:]
    group = jnp.broadcast_to(start // 8, low.shape)
    here = [group == place for place in range(groups)]
    rows = [
        jnp.where(here[place], low, jnp.where(here[place - 1], high, 0.0))
        for place in range(groups)
    ]
    return jnp.concatenate(rows, axis=0)


def bead_tables(cells, weights):
    first = hat_rows(SPAN_PAD, cells // (LY * LZ), weights[0:4], 0)
    second = hat_rows(SPAN_PAD, cells // LZ % LY, weights[4:8], 0)
    depth = depth_rows(cells % LZ, weights[8:12])
    return first, second, depth


def face_rows(first, second):
    inside = [first[row : row + 1] * second[:LY] for row in range(SPAN)]
    outside = [second[row : row + 1] * first for row in range(LY, SPAN)]
    return jnp.concatenate(inside + outside, axis=0)


def spread_kernel(
    count_ref,
    charge_ref,
    cell_ref,
    weight_ref,
    out_ref,
    up_ref,
    down_ref,
    depth_ref,
    first_ref,
    second_ref,
    total_ref,
    order_ref,
):
    step = pl.program_id(0)

    @pl.when(step == 0)
    def _():
        total_ref[...] = jnp.zeros_like(total_ref)

    dims = (((1,), (1,)), ((), ()))
    total = None
    for start in range(0, BLOCK, CHUNK):
        beads = slice(start, start + CHUNK)
        cells = cell_ref[0, :, beads]
        weights = weight_ref[0, 0, :, beads].astype(jnp.float32)
        first, second, depth = bead_tables(cells, weights)
        depth = depth.astype(jnp.bfloat16)
        depth_ref[:, beads] = depth
        first_ref[:, beads] = first
        second_ref[:, beads] = second
        slots = lax.broadcasted_iota(jnp.int32, cells.shape, 1) + (step * BLOCK + start)
        amount = jnp.where(slots < count_ref[0, 0], charge_ref[0, :, beads], 0.0)
        face = face_rows(first * amount, second)
        high = face.astype(jnp.bfloat16)
        low = (face - high.astype(jnp.float32)).astype(jnp.bfloat16)
        for term in (high, low):
            part = lax.dot_general(term, depth, dims, preferred_element_type=jnp.float32)
            total = part if total is None else total + part
    total_ref[...] += total

    @pl.when(step == pl.num_programs(0) - 1)
    def _():
        order_ref[...] = jnp.zeros_like(order_ref)
        for plane in range(SPAN):
            order_ref[plane * SPAN_PAD : plane * SPAN_PAD + LY] = total_ref[
                plane * LY : (plane + 1) * LY
            ]
        for column in range(SPAN - LY):
            start = SPAN * LY + column * SPAN_PAD
            order_ref[pl.ds(LY + column, SPAN_PAD, stride=SPAN_PAD)] = total_ref[
                start : start + SPAN_PAD
            ]
        out_ref[...] = order_ref[: SPAN * SPAN_PAD]
        up_ref[...] = order_ref[(SPAN - REACH) * SPAN_PAD : SPAN * SPAN_PAD].reshape(up_ref.shape)
        down_ref[...] = order_ref[: REACH * SPAN_PAD].reshape(down_ref.shape)


def read_kernel(count_ref, grid_ref, depth_ref, first_ref, second_ref, out_ref):
    step = pl.program_id(0)
    for start in range(0, BLOCK, READ_CHUNK):
        beads = slice(start, start + READ_CHUNK)
        depth = depth_ref[:, beads]
        along = jnp.dot(
            grid_ref[...],
            jnp.concatenate([depth, depth], axis=0),
            preferred_element_type=jnp.float32,
        )
        first = first_ref[:, beads]
        second = second_ref[:, beads]
        inside = first[0:1] * along[0:LY]
        for row in range(1, SPAN):
            inside = inside + first[row : row + 1] * along[row * LY : (row + 1) * LY]
        inside = inside * second[:LY]
        outside = None
        for column in range(SPAN - LY):
            place = SPAN * LY + column * SPAN_PAD
            part = second[LY + column : LY + column + 1] * along[place : place + SPAN_PAD]
            outside = part if outside is None else outside + part
        outside = outside * first
        parts = [inside[row : row + 8] for row in range(0, LY, 8)]
        parts += [outside[row : row + 8] for row in range(0, SPAN_PAD, 8)]
        picked = jnp.sum(sum(parts[1:], parts[0]), axis=0, keepdims=True)
        slots = lax.broadcasted_iota(jnp.int32, picked.shape, 1) + (step * BLOCK + start)
        out_ref[0, :, beads] = jnp.where(slots < count_ref[0, 0], picked, 0.0)


def whole_spec(shape):
    return pl.BlockSpec(shape, lambda i: (0,) * len(shape))


def table_specs():
    return [pl.BlockSpec((rows, BLOCK), lambda i: (0, i)) for rows in (LZ, SPAN_PAD, SPAN_PAD)]


def spread_beads(count, charge, cell, weights):
    slots = charge.shape[2]
    row = pl.BlockSpec((1, 1, BLOCK), lambda i: (0, 0, i))
    weight = pl.BlockSpec((1, 1, 12, BLOCK), lambda i: (0, 0, 0, i))
    edge = (REACH, SPAN_PAD, LZ)
    shapes = [
        jax.ShapeDtypeStruct((SPAN * SPAN_PAD, LZ), jnp.float32),
        jax.ShapeDtypeStruct(edge, jnp.float32),
        jax.ShapeDtypeStruct(edge, jnp.float32),
        jax.ShapeDtypeStruct((LZ, slots), jnp.bfloat16),
        jax.ShapeDtypeStruct((SPAN_PAD, slots), jnp.float32),
        jax.ShapeDtypeStruct((SPAN_PAD, slots), jnp.float32),
    ]
    return pl.pallas_call(
        spread_kernel,
        grid=(slots // BLOCK,),
        in_specs=[pl.BlockSpec(memory_space=pltpu.SMEM), row, row, weight],
        out_specs=[whole_spec(part.shape) for part in shapes[:3]] + table_specs(),
        out_shape=shapes,
        scratch_shapes=[
            pltpu.VMEM((FACE, LZ), jnp.float32),
            pltpu.VMEM((SPAN_PAD * SPAN_PAD, LZ), jnp.float32),
        ],
        name="spread",
        compiler_params=pltpu.CompilerParams(vmem_limit_bytes=VMEM_BYTES),
    )(count, charge, cell, weights)


def read_beads(count, grid, tables):
    slots = tables[0].shape[1]
    return pl.pallas_call(
        read_kernel,
        grid=(slots // BLOCK,),
        in_specs=[pl.BlockSpec(memory_space=pltpu.SMEM), whole_spec(grid.shape)] + table_specs(),
        out_specs=pl.BlockSpec((1, 1, BLOCK), lambda i: (0, 0, i)),
        out_shape=jax.ShapeDtypeStruct((1, 1, slots), jnp.float32),
        name="read",
        compiler_params=pltpu.CompilerParams(vmem_limit_bytes=VMEM_BYTES),
    )(count, grid, *tables)


def spline_of(distance, period):
    place = (distance + 2) & (period - 1)
    return jnp.where(
        place == 2,
        0.75,
        jnp.where(
            (place == 1) | (place == 3), 0.5, jnp.where((place == 0) | (place == 4), 0.125, 0.0)
        ),
    )


PERIOD = 32


def tap_rows(taps):
    side = taps.shape[0]
    tap = lax.broadcasted_iota(jnp.int32, (side, LZ), 0)
    lane = lax.broadcasted_iota(jnp.int32, (side, LZ), 1)
    table = jnp.where(((lane + tap - RADIUS) & (PERIOD - 1)) == 0, 1.0, 0.0).astype(jnp.bfloat16)
    return jnp.dot(taps, table, preferred_element_type=jnp.float32)


def turned(row):
    return pltpu.roll(
        jnp.broadcast_to(row, (PERIOD, row.shape[1])), 0, 1, stride=1, stride_axis=0
    )


def near_mask(rows, depth):
    row = lax.broadcasted_iota(jnp.int32, (rows, LZ), 0)
    lane = lax.broadcasted_iota(jnp.int32, (rows, LZ), 1)
    near = ((row - lane + RADIUS) & (depth - 1)) <= 2 * RADIUS
    return jnp.where(near, 1.0, 0.0).astype(jnp.bfloat16)


def three_terms(value):
    first = value.astype(jnp.bfloat16)
    rest = value - first.astype(jnp.float32)
    second = rest.astype(jnp.bfloat16)
    third = (rest - second.astype(jnp.float32)).astype(jnp.bfloat16)
    return first, second, third


def merged_plane(pieces, plane):
    own, below, above = pieces
    inner = plane - RADIUS
    if inner < 0:
        return below[plane]
    value = own[inner * SPAN_PAD : (inner + 1) * SPAN_PAD] if inner < SPAN else None
    if plane < REACH:
        return value + below[plane]
    if inner < LX:
        return value
    outer = above[inner - LX]
    return outer if value is None else value + outer


def gather_kernel(*refs):
    fine_ref, coarse_ref, up_ref, down_ref, half_ref = refs[-5:]
    own, before = refs[0:3], refs[3:6]
    after = before if len(refs) == 11 else refs[6:9]
    for plane in range(PLANES):
        middle = merged_plane(own, plane)
        lower = merged_plane(before, plane)
        upper = merged_plane(after, plane)
        value = jnp.concatenate(
            [
                lower[8:16],
                middle[0:8] + lower[16:24],
                middle[8:16],
                middle[16:24] + upper[0:8],
                upper[8:24],
            ],
            axis=0,
        )
        fine_ref[plane] = value.astype(jnp.bfloat16).astype(jnp.float32)
    spline = (0.125, 0.5, 0.75, 0.5, 0.125)
    for plane in range(KNOWN):
        total = spline[0] * fine_ref[2 * plane]
        for step in range(1, 5):
            total = total + spline[step] * fine_ref[2 * plane + step]
        half_ref[plane] = total
    total = spline[0] * half_ref[:, pl.ds(0, KNOWN, stride=2)]
    for step in range(1, 5):
        total = total + spline[step] * half_ref[:, pl.ds(step, KNOWN, stride=2)]
    terms = jnp.concatenate(three_terms(total.reshape(KNOWN * KNOWN, LZ)), axis=1)
    shape = (3 * LZ, LZ)
    fine_depth = lax.broadcasted_iota(jnp.int32, shape, 0) & (LZ - 1)
    coarse_depth = lax.broadcasted_iota(jnp.int32, shape, 1) & (HALF - 1)
    table = spline_of(fine_depth - 2 * coarse_depth, LZ).astype(jnp.bfloat16)
    coarse = jnp.dot(terms, table, preferred_element_type=jnp.float32)
    coarse = coarse.astype(jnp.bfloat16).reshape(coarse_ref.shape)
    coarse_ref[...] = coarse
    up_ref[...] = coarse[2 : 2 + EDGE]
    down_ref[...] = coarse[8 : 8 + EDGE]


def gather_fine(pieces):
    edge = jax.ShapeDtypeStruct((EDGE, KNOWN, LZ), jnp.bfloat16)
    return pl.pallas_call(
        gather_kernel,
        out_shape=(
            jax.ShapeDtypeStruct((PLANES, COLUMNS, LZ), jnp.float32),
            jax.ShapeDtypeStruct((KNOWN, KNOWN, LZ), jnp.bfloat16),
            edge,
            edge,
        ),
        scratch_shapes=[pltpu.VMEM((KNOWN, COLUMNS, LZ), jnp.float32)],
        name="gather",
        compiler_params=pltpu.CompilerParams(vmem_limit_bytes=VMEM_BYTES),
    )(*pieces)


def fine_kernel(
    fine_ref,
    tap_ref,
    coarse_tap_ref,
    out_ref,
    coarse_ref,
    pair_ref,
    row_ref,
    coarse_row_ref,
    even_ref,
    odd_ref,
):
    side = tap_ref.shape[0]
    row_ref[...] = jnp.zeros_like(row_ref)
    coarse_row_ref[...] = jnp.zeros_like(coarse_row_ref)
    for plane in range(side):
        row_ref[plane, 1 : 1 + side] = tap_rows(tap_ref[plane])
        coarse_row_ref[plane, 1 : 1 + side] = tap_rows(coarse_tap_ref[plane])
    for shift in range(SHIFTS):
        halves = [fine_ref[:, pl.ds(2 * shift + part, 16, stride=2)] for part in range(2)]
        pair_ref[shift] = (
            jnp.concatenate(halves, axis=2).reshape(PLANES * 16, 2 * LZ).astype(jnp.bfloat16)
        )
    out_ref[...] = jnp.zeros_like(out_ref)

    def build(table_ref, plane):
        mask = near_mask(LZ, LZ)
        for band in range(BANDS):
            block = turned(row_ref[plane, band : band + 1]).astype(jnp.bfloat16)
            table_ref[band] = jnp.concatenate([block] * (LZ // PERIOD), axis=0) * mask

    def build_coarse(index, part):
        plane = 2 * index + part
        lower_half = lax.broadcasted_iota(jnp.int32, (PERIOD, LZ), 1) < HALF
        mask = near_mask(HALF, HALF)
        before = turned(coarse_row_ref[plane, 0:1])
        for band in range(BANDS - 1):
            after = turned(coarse_row_ref[plane, band + 1 : band + 2])
            block = jnp.where(lower_half, after, before).astype(jnp.bfloat16)
            start = part * LZ + (band % 2) * HALF
            coarse_ref[index, band // 2, start : start + HALF] = (
                jnp.concatenate([block] * (HALF // PERIOD), axis=0) * mask
            )
            before = after

    def multiply(table_ref, plane):
        rows = pl.ds(pl.multiple_of(plane * 16, 16), SPAN * 16)
        total = out_ref[...]
        for shift in range(SHIFTS):
            band = 2 * shift + 1
            upper = jnp.concatenate([table_ref[band], table_ref[band - 1]], axis=1)
            lower = jnp.concatenate([table_ref[band + 1], table_ref[band]], axis=1)
            total = total + jnp.dot(
                pair_ref[shift, rows],
                jnp.concatenate([upper, lower], axis=0),
                preferred_element_type=jnp.float32,
            )
        out_ref[...] = total

    build(even_ref, 0)

    def two_planes(index, carry):
        plane = 2 * index
        build(odd_ref, plane + 1)
        build_coarse(index, 0)
        multiply(even_ref, plane)
        build(even_ref, plane + 2)
        build_coarse(index, 1)
        multiply(odd_ref, plane + 1)
        return carry

    lax.fori_loop(0, side // 2, two_planes, 0)
    build_coarse(side // 2, 0)
    build_coarse(side // 2, 1)
    multiply(even_ref, side - 1)


def fine_sums(fine, kernel, kernel_coarse):
    side = kernel.shape[0]
    pairs = (side + 1) // 2
    return pl.pallas_call(
        fine_kernel,
        out_shape=(
            jax.ShapeDtypeStruct((SPAN * 16, 2 * LZ), jnp.float32),
            jax.ShapeDtypeStruct((pairs, SHIFTS, 2 * LZ, LZ), jnp.bfloat16),
        ),
        scratch_shapes=[
            pltpu.VMEM((SHIFTS, PLANES * 16, 2 * LZ), jnp.bfloat16),
            pltpu.VMEM((side, SPAN_PAD, LZ), jnp.float32),
            pltpu.VMEM((2 * pairs, SPAN_PAD, LZ), jnp.float32),
            pltpu.VMEM((BANDS, LZ, LZ), jnp.bfloat16),
            pltpu.VMEM((BANDS, LZ, LZ), jnp.bfloat16),
        ],
        name="fine",
        compiler_params=pltpu.CompilerParams(vmem_limit_bytes=VMEM_BYTES),
    )(fine, kernel, kernel_coarse)


def coarse_kernel(
    own_ref,
    below_ref,
    above_ref,
    low_ref,
    high_ref,
    table_ref,
    sums_ref,
    grid_ref,
    face_ref,
    cell_ref,
    pair_ref,
    total_ref,
    coarse_ref,
    wide_ref,
    join_ref,
):
    step = pl.program_id(0)

    @pl.when(step == 0)
    def _():
        total_ref[...] = jnp.zeros_like(total_ref)
        cell_ref[...] = jnp.zeros_like(cell_ref)
        for start, part in ((0, below_ref), (EDGE, own_ref), (EDGE + KNOWN, above_ref)):
            planes = slice(start, start + part.shape[0])
            values = part[...].astype(jnp.float32)
            cell_ref[planes, 8:24] = values
            if low_ref is None:
                cell_ref[planes, 0:8] = values[:, 8:16]
                cell_ref[planes, 24:32] = values[:, 0:8]
            else:
                cell_ref[planes, 0:8] = low_ref[planes].astype(jnp.float32)
                cell_ref[planes, 24:32] = high_ref[planes].astype(jnp.float32)
        lower_half = lax.broadcasted_iota(jnp.int32, (COARSE_IN + 1, 8, LZ), 2) < HALF
        for shift in range(SHIFTS):
            pair = jnp.where(
                lower_half,
                cell_ref[:, pl.ds(2 * shift + 2, 8, stride=2)],
                cell_ref[:, pl.ds(2 * shift + 3, 8, stride=2)],
            )
            rows = COARSE_IN * 8
            pair_ref[shift] = jnp.concatenate(
                [pair[:COARSE_IN].reshape(rows, LZ), pair[1:].reshape(rows, LZ)], axis=1
            ).astype(jnp.bfloat16)

    rows = pl.ds(pl.multiple_of(step * 16, 16), COARSE_OUT * 8)
    total = total_ref[...]
    for shift in range(SHIFTS):
        total = total + jnp.dot(
            pair_ref[shift, rows], table_ref[0, shift], preferred_element_type=jnp.float32
        )
    total_ref[...] = total

    @pl.when(step == pl.num_programs(0) - 1)
    def _():
        high = total.astype(jnp.bfloat16)
        low = (total - high.astype(jnp.float32)).astype(jnp.bfloat16)
        shape = (2 * LZ, 2 * LZ)
        source = lax.broadcasted_iota(jnp.int32, shape, 0)
        target = lax.broadcasted_iota(jnp.int32, shape, 1)
        table = jnp.where(
            (source // HALF) % 2 == target // LZ,
            spline_of((target & (LZ - 1)) - 2 * (source & (HALF - 1)), LZ),
            0.0,
        ).astype(jnp.bfloat16)
        deep = jnp.dot(
            jnp.concatenate([high, low], axis=1), table, preferred_element_type=jnp.float32
        )
        for part in range(2):
            coarse_ref[:, pl.ds(part, 8, stride=2)] = deep[:, part * LZ : (part + 1) * LZ].reshape(
                COARSE_OUT, 8, LZ
            )
        wide_ref[...] = jnp.zeros_like(wide_ref)
        for plane in range(SPAN):
            middle = plane // 2 + 1
            if plane % 2:
                value = (coarse_ref[middle] + coarse_ref[middle + 1]) * 0.5
            else:
                value = (
                    coarse_ref[middle - 1] + 6.0 * coarse_ref[middle] + coarse_ref[middle + 1]
                ) * 0.125
            wide_ref[plane, 0:16] = value
        before = wide_ref[:, 0:16]
        middle = wide_ref[:, 1:17]
        after = wide_ref[:, 2:18]
        even = (before + 6.0 * middle + after) * 0.125
        odd = (middle + after) * 0.5
        sums = sums_ref[...].reshape(SPAN, 16, 2 * LZ)
        join_ref[...] = jnp.zeros_like(join_ref)
        for plane in range(SPAN):
            start = plane * 32
            join_ref[pl.ds(start, 16, stride=2)] = sums[plane, :, :LZ] + even[plane]
            join_ref[pl.ds(start + 1, 16, stride=2)] = sums[plane, :, LZ:] + odd[plane]
        for plane in range(LX):
            grid_ref[plane] = join_ref[plane * 32 : plane * 32 + LY]
        inside = [join_ref[plane * 32 : plane * 32 + LY] for plane in range(SPAN)]
        outside = [join_ref[pl.ds(column, SPAN_PAD, stride=32)] for column in range(LY, SPAN)]
        face = jnp.concatenate(inside + outside, axis=0)
        face_high = face.astype(jnp.bfloat16)
        face_low = (face - face_high.astype(jnp.float32)).astype(jnp.bfloat16)
        face_ref[:, :LZ] = face_high
        face_ref[:, LZ:] = face_low


def potentials(own, below, above, low, high, table, sums):
    def whole(value):
        return pl.BlockSpec(value.shape, lambda i: (0,) * value.ndim)

    given = [own, below, above] + ([] if low is None else [low, high])
    specs = [whole(value) for value in given]
    specs.append(pl.BlockSpec((1, SHIFTS, 2 * LZ, LZ), lambda i: (i, 0, 0, 0)))
    specs.append(whole(sums))

    def body(*refs):
        if low is None:
            refs = refs[:3] + (None, None) + refs[3:]
        coarse_kernel(*refs)

    return pl.pallas_call(
        body,
        grid=(table.shape[0],),
        in_specs=specs,
        out_specs=(
            pl.BlockSpec((LX, LY, LZ), lambda i: (0, 0, 0)),
            pl.BlockSpec((FACE, 2 * LZ), lambda i: (0, 0)),
        ),
        out_shape=(
            jax.ShapeDtypeStruct((LX, LY, LZ), jnp.float32),
            jax.ShapeDtypeStruct((FACE, 2 * LZ), jnp.bfloat16),
        ),
        scratch_shapes=[
            pltpu.VMEM((COARSE_IN + 1, 40, LZ), jnp.float32),
            pltpu.VMEM((SHIFTS, COARSE_IN * 8, 2 * LZ), jnp.bfloat16),
            pltpu.VMEM((COARSE_OUT * 8, LZ), jnp.float32),
            pltpu.VMEM((COARSE_OUT, 16, LZ), jnp.float32),
            pltpu.VMEM((SPAN, 24, LZ), jnp.float32),
            pltpu.VMEM((SPAN_PAD * 32, LZ), jnp.float32),
        ],
        name="coarse",
        compiler_params=pltpu.CompilerParams(vmem_limit_bytes=VMEM_BYTES),
    )(*given, table, sums)


def on_device(bead_charge, bead_cell, bead_count, interp_weights, kernel_fine, kernel_coarse):
    beads = [
        pltpu.with_memory_space_constraint(value, pltpu.HBM)
        for value in (bead_charge, bead_cell, interp_weights)
    ]
    own, up, down, *tables = spread_beads(bead_count, *beads)
    below = from_behind(up, "gx", 1)
    above = from_behind(down, "gx", -1)
    wraps = lax.axis_size("gy") == 2
    pieces = [own, below, above]
    for steps in (1,) if wraps else (1, -1):
        pieces += [from_behind(part, "gy", steps) for part in (own, below, above)]
    fine, coarse, coarse_up, coarse_down = gather_fine(pieces)
    coarse_below = from_behind(coarse_up, "gx", 1)
    coarse_above = from_behind(coarse_down, "gx", -1)
    sums, table_coarse = fine_sums(fine, kernel_fine, kernel_coarse)
    low = high = None
    if not wraps:
        joined = jnp.concatenate([coarse_below, coarse, coarse_above], axis=0)
        low = from_behind(joined[:, :8], "gy", 1)
        high = from_behind(joined[:, 8:], "gy", -1)
    potential_grid, face = potentials(
        coarse, coarse_below, coarse_above, low, high, table_coarse, sums
    )
    bead_potential = read_beads(bead_count, face, tables)
    return (bead_potential, potential_grid)


def solution(mesh):
    return jax.shard_map(
        on_device,
        mesh=mesh,
        in_specs=(
            P("gx", "gy", None),
            P("gx", "gy", None),
            P("gx", "gy"),
            P("gx", "gy", None, None),
            P(),
            P(),
        ),
        out_specs=(P("gx", "gy", None), P("gx", "gy", None)),
        check_vma=False,
    )
```

```python
import jax
import jax.numpy as jnp
from jax import lax
from jax.experimental import pallas as pl
from jax.experimental.pallas import tpu as pltpu
from jax.sharding import PartitionSpec as P

LX = 16
LY = 16
LZ = 128
RADIUS = 8

SPAN = LX + 3
SPAN_PAD = 24
BLOCK = 2048
CHUNK = 256
READ_CHUNK = 512
FACE = SPAN * LY + (SPAN - LY) * SPAN_PAD
VMEM_BYTES = 24 * 1024 * 1024
REACH = 11
PLANES = SPAN + 2 * RADIUS
PLANES_PAD = 40
COLUMNS = 48
NEAR = (SPAN + 1) * 8
FAR = 2 * SPAN_PAD
SHIFTS = RADIUS + 1
BANDS = 2 * RADIUS + 3
HALF = LZ // 2
KNOWN = 16
EDGE = 6
COARSE_OUT = 12
COARSE_IN = COARSE_OUT + 2 * RADIUS


def from_behind(value, axis, steps):
    count = lax.axis_size(axis)
    pairs = [(source, (source + steps) % count) for source in range(count)]
    return lax.ppermute(value, axis, pairs)


def hat_rows(rows, start, weights, period):
    places = lax.broadcasted_iota(jnp.int32, (rows, start.shape[1]), 0) - start
    if period:
        places = places & (period - 1)
    table = jnp.where(places == 3, weights[3:4], 0.0)
    for offset in (2, 1, 0):
        table = jnp.where(places == offset, weights[offset : offset + 1], table)
    return table


def depth_rows(start, weights):
    groups = LZ // 8
    pattern = hat_rows(16, start & 7, weights, 0)
    low, high = pattern[:8], pattern[8:]
    group = jnp.broadcast_to(start // 8, low.shape)
    here = [group == place for place in range(groups)]
    rows = [
        jnp.where(here[place], low, jnp.where(here[place - 1], high, 0.0))
        for place in range(groups)
    ]
    return jnp.concatenate(rows, axis=0)


def bead_tables(cells, weights):
    first = hat_rows(SPAN_PAD, cells // (LY * LZ), weights[0:4], 0)
    second = hat_rows(SPAN_PAD, cells // LZ % LY, weights[4:8], 0)
    depth = depth_rows(cells % LZ, weights[8:12])
    return first, second, depth


def face_rows(first, second):
    inside = [first[row : row + 1] * second[:LY] for row in range(SPAN)]
    outside = [second[row : row + 1] * first for row in range(LY, SPAN)]
    return jnp.concatenate(inside + outside, axis=0)


def spread_kernel(
    count_ref,
    charge_ref,
    cell_ref,
    weight_ref,
    tap_ref,
    coarse_tap_ref,
    out_ref,
    up_ref,
    down_ref,
    depth_ref,
    first_ref,
    second_ref,
    row_ref,
    coarse_row_ref,
    total_ref,
    order_ref,
):
    step = pl.program_id(0)

    @pl.when(step == 0)
    def _():
        total_ref[...] = jnp.zeros_like(total_ref)
        row_ref[...] = jnp.zeros_like(row_ref)
        coarse_row_ref[...] = jnp.zeros_like(coarse_row_ref)
        side = tap_ref.shape[0]
        for plane in range(side):
            row_ref[plane, 1 : 1 + side] = tap_rows(tap_ref[plane])
            coarse_row_ref[plane, 1 : 1 + side] = tap_rows(coarse_tap_ref[plane])

    dims = (((1,), (1,)), ((), ()))
    total = None
    for start in range(0, BLOCK, CHUNK):
        beads = slice(start, start + CHUNK)
        cells = cell_ref[0, :, beads]
        weights = weight_ref[0, 0, :, beads].astype(jnp.float32)
        first, second, depth = bead_tables(cells, weights)
        depth = depth.astype(jnp.bfloat16)
        kept = pl.ds(pl.multiple_of(step * BLOCK, BLOCK) + start, CHUNK)
        depth_ref[:, kept] = depth
        first_ref[:, kept] = first
        second_ref[:, kept] = second
        slots = lax.broadcasted_iota(jnp.int32, cells.shape, 1) + (step * BLOCK + start)
        amount = jnp.where(slots < count_ref[0, 0], charge_ref[0, :, beads], 0.0)
        face = face_rows(first * amount, second)
        high = face.astype(jnp.bfloat16)
        low = (face - high.astype(jnp.float32)).astype(jnp.bfloat16)
        for term in (high, low):
            part = lax.dot_general(term, depth, dims, preferred_element_type=jnp.float32)
            total = part if total is None else total + part
    total_ref[...] += total

    @pl.when(step == pl.num_programs(0) - 1)
    def _():
        order_ref[...] = jnp.zeros_like(order_ref)
        for plane in range(SPAN):
            order_ref[plane * SPAN_PAD : plane * SPAN_PAD + LY] = total_ref[
                plane * LY : (plane + 1) * LY
            ]
        for column in range(SPAN - LY):
            start = SPAN * LY + column * SPAN_PAD
            order_ref[pl.ds(LY + column, SPAN_PAD, stride=SPAN_PAD)] = total_ref[
                start : start + SPAN_PAD
            ]
        out_ref[...] = order_ref[: SPAN * SPAN_PAD]
        up_ref[...] = order_ref[(SPAN - REACH) * SPAN_PAD : SPAN * SPAN_PAD].reshape(up_ref.shape)
        down_ref[...] = order_ref[: REACH * SPAN_PAD].reshape(down_ref.shape)


def read_kernel(count_ref, grid_ref, depth_ref, first_ref, second_ref, out_ref):
    step = pl.program_id(0)
    for start in range(0, BLOCK, READ_CHUNK):
        beads = slice(start, start + READ_CHUNK)
        kept = pl.ds(pl.multiple_of(step * BLOCK, BLOCK) + start, READ_CHUNK)
        depth = depth_ref[:, kept]
        along = jnp.dot(
            grid_ref[...],
            jnp.concatenate([depth, depth], axis=0),
            preferred_element_type=jnp.float32,
        )
        first = first_ref[:, kept]
        second = second_ref[:, kept]
        inside = first[0:1] * along[0:LY]
        for row in range(1, SPAN):
            inside = inside + first[row : row + 1] * along[row * LY : (row + 1) * LY]
        inside = inside * second[:LY]
        outside = None
        for column in range(SPAN - LY):
            place = SPAN * LY + column * SPAN_PAD
            part = second[LY + column : LY + column + 1] * along[place : place + SPAN_PAD]
            outside = part if outside is None else outside + part
        outside = outside * first
        parts = [inside[row : row + 8] for row in range(0, LY, 8)]
        parts += [outside[row : row + 8] for row in range(0, SPAN_PAD, 8)]
        picked = jnp.sum(sum(parts[1:], parts[0]), axis=0, keepdims=True)
        slots = lax.broadcasted_iota(jnp.int32, picked.shape, 1) + (step * BLOCK + start)
        out_ref[0, :, beads] = jnp.where(slots < count_ref[0, 0], picked, 0.0)


def whole_spec(shape):
    return pl.BlockSpec(shape, lambda i: (0,) * len(shape))


def table_specs():
    return [pl.BlockSpec(memory_space=pltpu.VMEM)] * 3


def spread_beads(count, charge, cell, weights, kernel, kernel_coarse):
    slots = charge.shape[2]
    row = pl.BlockSpec((1, 1, BLOCK), lambda i: (0, 0, i))
    weight = pl.BlockSpec((1, 1, 12, BLOCK), lambda i: (0, 0, 0, i))
    edge = (REACH, SPAN_PAD, LZ)
    side = kernel.shape[0]
    shapes = [
        jax.ShapeDtypeStruct((SPAN * SPAN_PAD, LZ), jnp.float32),
        jax.ShapeDtypeStruct(edge, jnp.float32),
        jax.ShapeDtypeStruct(edge, jnp.float32),
        jax.ShapeDtypeStruct((LZ, slots), jnp.bfloat16),
        jax.ShapeDtypeStruct((SPAN_PAD, slots), jnp.float32),
        jax.ShapeDtypeStruct((SPAN_PAD, slots), jnp.float32),
        jax.ShapeDtypeStruct((side, SPAN_PAD, LZ), jnp.float32),
        jax.ShapeDtypeStruct((side + 1, SPAN_PAD, LZ), jnp.float32),
    ]
    tap_specs = [whole_spec(kernel.shape)] * 2
    return pl.pallas_call(
        spread_kernel,
        grid=(slots // BLOCK,),
        in_specs=[pl.BlockSpec(memory_space=pltpu.SMEM), row, row, weight] + tap_specs,
        out_specs=[whole_spec(part.shape) for part in shapes[:3]]
        + table_specs()
        + [whole_spec(part.shape) for part in shapes[6:]],
        out_shape=shapes,
        scratch_shapes=[
            pltpu.VMEM((FACE, LZ), jnp.float32),
            pltpu.VMEM((SPAN_PAD * SPAN_PAD, LZ), jnp.float32),
        ],
        name="spread",
        compiler_params=pltpu.CompilerParams(vmem_limit_bytes=VMEM_BYTES),
    )(count, charge, cell, weights, kernel, kernel_coarse)


def read_beads(count, grid, tables):
    slots = tables[0].shape[1]
    return pl.pallas_call(
        read_kernel,
        grid=(slots // BLOCK,),
        in_specs=[pl.BlockSpec(memory_space=pltpu.SMEM), whole_spec(grid.shape)] + table_specs(),
        out_specs=pl.BlockSpec((1, 1, BLOCK), lambda i: (0, 0, i)),
        out_shape=jax.ShapeDtypeStruct((1, 1, slots), jnp.float32),
        name="read",
        compiler_params=pltpu.CompilerParams(vmem_limit_bytes=VMEM_BYTES),
    )(count, grid, *tables)


def spline_of(distance, period):
    place = (distance + 2) & (period - 1)
    return jnp.where(
        place == 2,
        0.75,
        jnp.where(
            (place == 1) | (place == 3), 0.5, jnp.where((place == 0) | (place == 4), 0.125, 0.0)
        ),
    )


PERIOD = 32


def tap_rows(taps):
    side = taps.shape[0]
    tap = lax.broadcasted_iota(jnp.int32, (side, LZ), 0)
    lane = lax.broadcasted_iota(jnp.int32, (side, LZ), 1)
    table = jnp.where(((lane + tap - RADIUS) & (PERIOD - 1)) == 0, 1.0, 0.0).astype(jnp.bfloat16)
    return jnp.dot(taps, table, preferred_element_type=jnp.float32)


def turned(row):
    return pltpu.roll(
        jnp.broadcast_to(row, (PERIOD, row.shape[1])), 0, 1, stride=1, stride_axis=0
    )


def near_mask(rows, depth):
    row = lax.broadcasted_iota(jnp.int32, (rows, LZ), 0)
    lane = lax.broadcasted_iota(jnp.int32, (rows, LZ), 1)
    near = ((row - lane + RADIUS) & (depth - 1)) <= 2 * RADIUS
    return jnp.where(near, 1.0, 0.0).astype(jnp.bfloat16)


def three_terms(value):
    first = value.astype(jnp.bfloat16)
    rest = value - first.astype(jnp.float32)
    second = rest.astype(jnp.bfloat16)
    third = (rest - second.astype(jnp.float32)).astype(jnp.bfloat16)
    return first, second, third


def merged_plane(pieces, plane):
    own, below, above = pieces
    inner = plane - RADIUS
    if inner < 0:
        return below[plane]
    value = own[inner * SPAN_PAD : (inner + 1) * SPAN_PAD] if inner < SPAN else None
    if plane < REACH:
        return value + below[plane]
    if inner < LX:
        return value
    outer = above[inner - LX]
    return outer if value is None else value + outer


def gather_kernel(*refs):
    fine_ref, coarse_ref, up_ref, down_ref, half_ref = refs[-5:]
    own, before = refs[0:3], refs[3:6]
    after = before if len(refs) == 11 else refs[6:9]
    for plane in range(PLANES):
        middle = merged_plane(own, plane)
        lower = merged_plane(before, plane)
        upper = merged_plane(after, plane)
        value = jnp.concatenate(
            [
                lower[8:16],
                middle[0:8] + lower[16:24],
                middle[8:16],
                middle[16:24] + upper[0:8],
                upper[8:24],
            ],
            axis=0,
        )
        fine_ref[plane] = value.astype(jnp.bfloat16).astype(jnp.float32)
    fine_ref[PLANES:] = jnp.zeros_like(fine_ref[PLANES:])
    spline = (0.125, 0.5, 0.75, 0.5, 0.125)
    for plane in range(KNOWN):
        total = spline[0] * fine_ref[2 * plane]
        for step in range(1, 5):
            total = total + spline[step] * fine_ref[2 * plane + step]
        half_ref[plane] = total
    total = spline[0] * half_ref[:, pl.ds(0, KNOWN, stride=2)]
    for step in range(1, 5):
        total = total + spline[step] * half_ref[:, pl.ds(step, KNOWN, stride=2)]
    terms = jnp.concatenate(three_terms(total.reshape(KNOWN * KNOWN, LZ)), axis=1)
    shape = (3 * LZ, LZ)
    fine_depth = lax.broadcasted_iota(jnp.int32, shape, 0) & (LZ - 1)
    coarse_depth = lax.broadcasted_iota(jnp.int32, shape, 1) & (HALF - 1)
    table = spline_of(fine_depth - 2 * coarse_depth, LZ).astype(jnp.bfloat16)
    coarse = jnp.dot(terms, table, preferred_element_type=jnp.float32)
    coarse = coarse.astype(jnp.bfloat16).reshape(coarse_ref.shape)
    coarse_ref[...] = coarse
    up_ref[...] = coarse[2 : 2 + EDGE]
    down_ref[...] = coarse[8 : 8 + EDGE]


def gather_fine(pieces):
    edge = jax.ShapeDtypeStruct((EDGE, KNOWN, LZ), jnp.bfloat16)
    return pl.pallas_call(
        gather_kernel,
        out_shape=(
            jax.ShapeDtypeStruct((PLANES_PAD, COLUMNS, LZ), jnp.float32),
            jax.ShapeDtypeStruct((KNOWN, KNOWN, LZ), jnp.bfloat16),
            edge,
            edge,
        ),
        scratch_shapes=[pltpu.VMEM((KNOWN, COLUMNS, LZ), jnp.float32)],
        name="gather",
        compiler_params=pltpu.CompilerParams(vmem_limit_bytes=VMEM_BYTES),
    )(*pieces)


def fine_kernel(
    fine_ref,
    row_ref,
    coarse_row_ref,
    out_ref,
    coarse_ref,
    pair_ref,
    even_ref,
    odd_ref,
):
    side = row_ref.shape[0]
    flat_ref = fine_ref.reshape(PLANES_PAD * COLUMNS, LZ)
    kept = pair_ref.shape[2] // 8
    for shift in range(SHIFTS):
        halves = [fine_ref[:, pl.ds(2 * shift + part, 8, stride=2)] for part in range(2)]
        both = jnp.concatenate(halves, axis=2)
        for part in range(2):
            pair_ref[part, shift] = (
                both[part : part + kept].reshape(kept * 8, 2 * LZ).astype(jnp.bfloat16)
            )
    out_ref[...] = jnp.zeros_like(out_ref)

    def build(table_ref, plane):
        mask = near_mask(LZ, LZ)
        for band in range(BANDS):
            block = turned(row_ref[plane, band : band + 1]).astype(jnp.bfloat16)
            table_ref[band] = jnp.concatenate([block] * (LZ // PERIOD), axis=0) * mask

    def build_coarse(index, part):
        plane = 2 * index + part
        lower_half = lax.broadcasted_iota(jnp.int32, (PERIOD, LZ), 1) < HALF
        mask = near_mask(HALF, HALF)
        before = turned(coarse_row_ref[plane, 0:1])
        for band in range(BANDS - 1):
            after = turned(coarse_row_ref[plane, band + 1 : band + 2])
            block = jnp.where(lower_half, after, before).astype(jnp.bfloat16)
            start = part * LZ + (band % 2) * HALF
            coarse_ref[index, band // 2, start : start + HALF] = (
                jnp.concatenate([block] * (HALF // PERIOD), axis=0) * mask
            )
            before = after

    def multiply(table_ref, plane, part):
        rows = pl.ds(pl.multiple_of((plane - part) * 8, 16), NEAR)
        far = []
        for pair in range(SHIFTS + 1):
            column = plane * COLUMNS + LY + 2 * pair
            halves = [
                flat_ref[pl.ds(column + half, SPAN_PAD, stride=COLUMNS)] for half in range(2)
            ]
            far.append(jnp.concatenate(halves, axis=1))
        total = out_ref[...]
        for shift in range(SHIFTS):
            band = 2 * shift + 1
            upper = jnp.concatenate([table_ref[band], table_ref[band - 1]], axis=1)
            lower = jnp.concatenate([table_ref[band + 1], table_ref[band]], axis=1)
            outer = jnp.concatenate(far[shift : shift + 2], axis=0).astype(jnp.bfloat16)
            total = total + jnp.dot(
                jnp.concatenate([pair_ref[part, shift, rows], outer], axis=0),
                jnp.concatenate([upper, lower], axis=0),
                preferred_element_type=jnp.float32,
            )
        out_ref[...] = total

    build(even_ref, 0)

    def two_planes(index, carry):
        plane = 2 * index
        build(odd_ref, plane + 1)
        build_coarse(index, 0)
        multiply(even_ref, plane, 0)
        build(even_ref, plane + 2)
        build_coarse(index, 1)
        multiply(odd_ref, plane + 1, 1)
        return carry

    lax.fori_loop(0, side // 2, two_planes, 0)
    build_coarse(side // 2, 0)
    build_coarse(side // 2, 1)
    multiply(even_ref, side - 1, 0)


def fine_sums(fine, rows, rows_coarse):
    side = rows.shape[0]
    pairs = (side + 1) // 2
    return pl.pallas_call(
        fine_kernel,
        out_shape=(
            jax.ShapeDtypeStruct((NEAR + FAR, 2 * LZ), jnp.float32),
            jax.ShapeDtypeStruct((pairs, SHIFTS, 2 * LZ, LZ), jnp.bfloat16),
        ),
        scratch_shapes=[
            pltpu.VMEM((2, SHIFTS, NEAR + 16 * RADIUS, 2 * LZ), jnp.bfloat16),
            pltpu.VMEM((BANDS, LZ, LZ), jnp.bfloat16),
            pltpu.VMEM((BANDS, LZ, LZ), jnp.bfloat16),
        ],
        name="fine",
        compiler_params=pltpu.CompilerParams(vmem_limit_bytes=VMEM_BYTES),
    )(fine, rows, rows_coarse)


def coarse_kernel(
    own_ref,
    below_ref,
    above_ref,
    low_ref,
    high_ref,
    table_ref,
    sums_ref,
    grid_ref,
    face_ref,
    cell_ref,
    pair_ref,
    total_ref,
    coarse_ref,
    wide_ref,
    join_ref,
):
    step = pl.program_id(0)

    @pl.when(step == 0)
    def _():
        total_ref[...] = jnp.zeros_like(total_ref)
        cell_ref[...] = jnp.zeros_like(cell_ref)
        for start, part in ((0, below_ref), (EDGE, own_ref), (EDGE + KNOWN, above_ref)):
            planes = slice(start, start + part.shape[0])
            values = part[...].astype(jnp.float32)
            cell_ref[planes, 8:24] = values
            if low_ref is None:
                cell_ref[planes, 0:8] = values[:, 8:16]
                cell_ref[planes, 24:32] = values[:, 0:8]
            else:
                cell_ref[planes, 0:8] = low_ref[planes].astype(jnp.float32)
                cell_ref[planes, 24:32] = high_ref[planes].astype(jnp.float32)
        lower_half = lax.broadcasted_iota(jnp.int32, (COARSE_IN + 1, 8, LZ), 2) < HALF
        for shift in range(SHIFTS):
            pair = jnp.where(
                lower_half,
                cell_ref[:, pl.ds(2 * shift + 2, 8, stride=2)],
                cell_ref[:, pl.ds(2 * shift + 3, 8, stride=2)],
            )
            rows = COARSE_IN * 8
            pair_ref[shift] = jnp.concatenate(
                [pair[:COARSE_IN].reshape(rows, LZ), pair[1:].reshape(rows, LZ)], axis=1
            ).astype(jnp.bfloat16)

    rows = pl.ds(pl.multiple_of(step * 16, 16), COARSE_OUT * 8)
    total = total_ref[...]
    for shift in range(SHIFTS):
        total = total + jnp.dot(
            pair_ref[shift, rows], table_ref[0, shift], preferred_element_type=jnp.float32
        )
    total_ref[...] = total

    @pl.when(step == pl.num_programs(0) - 1)
    def _():
        high = total.astype(jnp.bfloat16)
        low = (total - high.astype(jnp.float32)).astype(jnp.bfloat16)
        shape = (2 * LZ, 2 * LZ)
        source = lax.broadcasted_iota(jnp.int32, shape, 0)
        target = lax.broadcasted_iota(jnp.int32, shape, 1)
        table = jnp.where(
            (source // HALF) % 2 == target // LZ,
            spline_of((target & (LZ - 1)) - 2 * (source & (HALF - 1)), LZ),
            0.0,
        ).astype(jnp.bfloat16)
        deep = jnp.dot(
            jnp.concatenate([high, low], axis=1), table, preferred_element_type=jnp.float32
        )
        for part in range(2):
            coarse_ref[:, pl.ds(part, 8, stride=2)] = deep[:, part * LZ : (part + 1) * LZ].reshape(
                COARSE_OUT, 8, LZ
            )
        wide_ref[...] = jnp.zeros_like(wide_ref)
        for plane in range(SPAN):
            middle = plane // 2 + 1
            if plane % 2:
                value = (coarse_ref[middle] + coarse_ref[middle + 1]) * 0.5
            else:
                value = (
                    coarse_ref[middle - 1] + 6.0 * coarse_ref[middle] + coarse_ref[middle + 1]
                ) * 0.125
            wide_ref[plane, 0:16] = value
        before = wide_ref[:, 0:16]
        middle = wide_ref[:, 1:17]
        after = wide_ref[:, 2:18]
        even = (before + 6.0 * middle + after) * 0.125
        odd = (middle + after) * 0.5
        near = sums_ref[:NEAR].reshape(SPAN + 1, 8, 2 * LZ)
        join_ref[...] = jnp.zeros_like(join_ref)
        for plane in range(SPAN):
            start = plane * 32
            for part, refined in ((0, even[plane]), (1, odd[plane])):
                join_ref[pl.ds(start + part, 8, stride=2)] = (
                    near[plane, :, part * LZ : (part + 1) * LZ] + refined[:8]
                )
                join_ref[pl.ds(start + 16 + part, 8, stride=2)] = refined[8:]
        for column in range(LY, SPAN):
            pair, part = divmod(column - LY, 2)
            rows = slice(NEAR + pair * SPAN_PAD, NEAR + (pair + 1) * SPAN_PAD)
            join_ref[pl.ds(column, SPAN_PAD, stride=32)] += sums_ref[
                rows, part * LZ : (part + 1) * LZ
            ]
        for plane in range(LX):
            grid_ref[plane] = join_ref[plane * 32 : plane * 32 + LY]
        inside = [join_ref[plane * 32 : plane * 32 + LY] for plane in range(SPAN)]
        outside = [join_ref[pl.ds(column, SPAN_PAD, stride=32)] for column in range(LY, SPAN)]
        face = jnp.concatenate(inside + outside, axis=0)
        face_high = face.astype(jnp.bfloat16)
        face_low = (face - face_high.astype(jnp.float32)).astype(jnp.bfloat16)
        face_ref[:, :LZ] = face_high
        face_ref[:, LZ:] = face_low


def potentials(own, below, above, low, high, table, sums):
    def whole(value):
        return pl.BlockSpec(value.shape, lambda i: (0,) * value.ndim)

    given = [own, below, above] + ([] if low is None else [low, high])
    specs = [whole(value) for value in given]
    specs.append(pl.BlockSpec((1, SHIFTS, 2 * LZ, LZ), lambda i: (i, 0, 0, 0)))
    specs.append(whole(sums))

    def body(*refs):
        if low is None:
            refs = refs[:3] + (None, None) + refs[3:]
        coarse_kernel(*refs)

    return pl.pallas_call(
        body,
        grid=(table.shape[0],),
        in_specs=specs,
        out_specs=(
            pl.BlockSpec((LX, LY, LZ), lambda i: (0, 0, 0)),
            pl.BlockSpec((FACE, 2 * LZ), lambda i: (0, 0)),
        ),
        out_shape=(
            jax.ShapeDtypeStruct((LX, LY, LZ), jnp.float32),
            jax.ShapeDtypeStruct((FACE, 2 * LZ), jnp.bfloat16),
        ),
        scratch_shapes=[
            pltpu.VMEM((COARSE_IN + 1, 40, LZ), jnp.float32),
            pltpu.VMEM((SHIFTS, COARSE_IN * 8, 2 * LZ), jnp.bfloat16),
            pltpu.VMEM((COARSE_OUT * 8, LZ), jnp.float32),
            pltpu.VMEM((COARSE_OUT, 16, LZ), jnp.float32),
            pltpu.VMEM((SPAN, 24, LZ), jnp.float32),
            pltpu.VMEM((SPAN_PAD * 32, LZ), jnp.float32),
        ],
        name="coarse",
        compiler_params=pltpu.CompilerParams(vmem_limit_bytes=VMEM_BYTES),
    )(*given, table, sums)


def on_device(bead_charge, bead_cell, bead_count, interp_weights, kernel_fine, kernel_coarse):
    beads = [
        pltpu.with_memory_space_constraint(value, pltpu.HBM)
        for value in (bead_charge, bead_cell, interp_weights, kernel_fine, kernel_coarse)
    ]
    own, up, down, *tables, rows, rows_coarse = spread_beads(bead_count, *beads)
    below = from_behind(up, "gx", 1)
    above = from_behind(down, "gx", -1)
    wraps = lax.axis_size("gy") == 2
    pieces = [own, below, above]
    for steps in (1,) if wraps else (1, -1):
        pieces += [from_behind(part, "gy", steps) for part in (own, below, above)]
    fine, coarse, coarse_up, coarse_down = gather_fine(pieces)
    coarse_below = from_behind(coarse_up, "gx", 1)
    coarse_above = from_behind(coarse_down, "gx", -1)
    sums, table_coarse = fine_sums(fine, rows, rows_coarse)
    low = high = None
    if not wraps:
        joined = jnp.concatenate([coarse_below, coarse, coarse_above], axis=0)
        low = from_behind(joined[:, :8], "gy", 1)
        high = from_behind(joined[:, 8:], "gy", -1)
    potential_grid, face = potentials(
        coarse, coarse_below, coarse_above, low, high, table_coarse, sums
    )
    bead_potential = read_beads(bead_count, face, tables)
    return (bead_potential, potential_grid)


def solution(mesh):
    return jax.shard_map(
        on_device,
        mesh=mesh,
        in_specs=(
            P("gx", "gy", None),
            P("gx", "gy", None),
            P("gx", "gy"),
            P("gx", "gy", None, None),
            P(),
            P(),
        ),
        out_specs=(P("gx", "gy", None), P("gx", "gy", None)),
        check_vma=False,
    )
```

```python
import jax
import jax.numpy as jnp
from jax import lax
from jax.experimental import pallas as pl
from jax.experimental.pallas import tpu as pltpu
from jax.sharding import PartitionSpec as P

LX = 16
LY = 16
LZ = 128
RADIUS = 8

SPAN = LX + 3
SPAN_PAD = 24
BLOCK = 4096
CHUNK = 256
READ_CHUNK = 512
READ_BLOCK = 8192
FACE = SPAN * LY + (SPAN - LY) * SPAN_PAD
VMEM_BYTES = 24 * 1024 * 1024
REACH = 11
PLANES = SPAN + 2 * RADIUS
PLANES_PAD = 40
COLUMNS = 48
NEAR = (SPAN + 1) * 8
FAR = 2 * SPAN_PAD
SHIFTS = RADIUS + 1
BANDS = 2 * RADIUS + 3
HALF = LZ // 2
KNOWN = 16
EDGE = 6
COARSE_OUT = 12
COARSE_IN = COARSE_OUT + 2 * RADIUS


def from_behind(value, axis, steps):
    count = lax.axis_size(axis)
    pairs = [(source, (source + steps) % count) for source in range(count)]
    return lax.ppermute(value, axis, pairs)


def hat_rows(rows, start, weights, period):
    places = lax.broadcasted_iota(jnp.int32, (rows, start.shape[1]), 0) - start
    if period:
        places = places & (period - 1)
    table = jnp.where(places == 3, weights[3:4], 0.0)
    for offset in (2, 1, 0):
        table = jnp.where(places == offset, weights[offset : offset + 1], table)
    return table


def depth_rows(start, weights):
    groups = LZ // 8
    pattern = hat_rows(16, start & 7, weights, 0)
    low, high = pattern[:8], pattern[8:]
    group = jnp.broadcast_to(start // 8, low.shape)
    here = [group == place for place in range(groups)]
    rows = [
        jnp.where(here[place], low, jnp.where(here[place - 1], high, 0.0))
        for place in range(groups)
    ]
    return jnp.concatenate(rows, axis=0)


def bead_tables(cells, weights):
    first = hat_rows(SPAN_PAD, cells // (LY * LZ), weights[0:4], 0)
    second = hat_rows(SPAN_PAD, cells // LZ % LY, weights[4:8], 0)
    depth = depth_rows(cells % LZ, weights[8:12])
    return first, second, depth


def face_rows(first, second):
    inside = [first[row : row + 1] * second[:LY] for row in range(SPAN)]
    outside = [second[row : row + 1] * first for row in range(LY, SPAN)]
    return jnp.concatenate(inside + outside, axis=0)


def spread_kernel(
    count_ref,
    charge_ref,
    cell_ref,
    weight_ref,
    tap_ref,
    coarse_tap_ref,
    out_ref,
    up_ref,
    down_ref,
    depth_ref,
    first_ref,
    second_ref,
    row_ref,
    coarse_row_ref,
    total_ref,
    order_ref,
):
    step = pl.program_id(0)

    @pl.when(step == 0)
    def _():
        total_ref[...] = jnp.zeros_like(total_ref)
        row_ref[...] = jnp.zeros_like(row_ref)
        coarse_row_ref[...] = jnp.zeros_like(coarse_row_ref)
        side = tap_ref.shape[0]
        for plane in range(side):
            row_ref[plane, 1 : 1 + side] = tap_rows(tap_ref[plane])
            coarse_row_ref[plane, 1 : 1 + side] = tap_rows(coarse_tap_ref[plane])

    dims = (((1,), (1,)), ((), ()))
    total = None
    for start in range(0, BLOCK, CHUNK):
        beads = slice(start, start + CHUNK)
        cells = cell_ref[0, :, beads]
        weights = weight_ref[0, 0, :, beads].astype(jnp.float32)
        first, second, depth = bead_tables(cells, weights)
        depth = depth.astype(jnp.bfloat16)
        kept = pl.ds(pl.multiple_of(step * BLOCK, BLOCK) + start, CHUNK)
        depth_ref[:, kept] = depth
        first_ref[:, kept] = first
        second_ref[:, kept] = second
        slots = lax.broadcasted_iota(jnp.int32, cells.shape, 1) + (step * BLOCK + start)
        amount = jnp.where(slots < count_ref[0, 0], charge_ref[0, :, beads], 0.0)
        face = face_rows(first * amount, second)
        high = face.astype(jnp.bfloat16)
        low = (face - high.astype(jnp.float32)).astype(jnp.bfloat16)
        for term in (high, low):
            part = lax.dot_general(term, depth, dims, preferred_element_type=jnp.float32)
            total = part if total is None else total + part
    total_ref[...] += total

    @pl.when(step == pl.num_programs(0) - 1)
    def _():
        order_ref[...] = jnp.zeros_like(order_ref)
        for plane in range(SPAN):
            order_ref[plane * SPAN_PAD : plane * SPAN_PAD + LY] = total_ref[
                plane * LY : (plane + 1) * LY
            ]
        for column in range(SPAN - LY):
            start = SPAN * LY + column * SPAN_PAD
            order_ref[pl.ds(LY + column, SPAN_PAD, stride=SPAN_PAD)] = total_ref[
                start : start + SPAN_PAD
            ]
        out_ref[...] = order_ref[: SPAN * SPAN_PAD]
        up_ref[...] = order_ref[(SPAN - REACH) * SPAN_PAD : SPAN * SPAN_PAD].reshape(up_ref.shape)
        down_ref[...] = order_ref[: REACH * SPAN_PAD].reshape(down_ref.shape)


def read_kernel(count_ref, grid_ref, depth_ref, first_ref, second_ref, out_ref):
    step = pl.program_id(0)
    for start in range(0, READ_BLOCK, READ_CHUNK):
        beads = slice(start, start + READ_CHUNK)
        kept = pl.ds(pl.multiple_of(step * READ_BLOCK, READ_BLOCK) + start, READ_CHUNK)
        depth = depth_ref[:, kept]
        along = jnp.dot(
            grid_ref[...],
            jnp.concatenate([depth, depth], axis=0),
            preferred_element_type=jnp.float32,
        )
        first = first_ref[:, kept]
        second = second_ref[:, kept]
        inside = first[0:1] * along[0:LY]
        for row in range(1, SPAN):
            inside = inside + first[row : row + 1] * along[row * LY : (row + 1) * LY]
        inside = inside * second[:LY]
        outside = None
        for column in range(SPAN - LY):
            place = SPAN * LY + column * SPAN_PAD
            part = second[LY + column : LY + column + 1] * along[place : place + SPAN_PAD]
            outside = part if outside is None else outside + part
        outside = outside * first
        parts = [inside[row : row + 8] for row in range(0, LY, 8)]
        parts += [outside[row : row + 8] for row in range(0, SPAN_PAD, 8)]
        picked = jnp.sum(sum(parts[1:], parts[0]), axis=0, keepdims=True)
        slots = lax.broadcasted_iota(jnp.int32, picked.shape, 1) + (step * READ_BLOCK + start)
        out_ref[0, :, beads] = jnp.where(slots < count_ref[0, 0], picked, 0.0)


def whole_spec(shape):
    return pl.BlockSpec(shape, lambda i: (0,) * len(shape))


def table_specs():
    return [pl.BlockSpec(memory_space=pltpu.VMEM)] * 3


def spread_beads(count, charge, cell, weights, kernel, kernel_coarse):
    slots = charge.shape[2]
    row = pl.BlockSpec((1, 1, BLOCK), lambda i: (0, 0, i))
    weight = pl.BlockSpec((1, 1, 12, BLOCK), lambda i: (0, 0, 0, i))
    edge = (REACH, SPAN_PAD, LZ)
    side = kernel.shape[0]
    shapes = [
        jax.ShapeDtypeStruct((SPAN * SPAN_PAD, LZ), jnp.float32),
        jax.ShapeDtypeStruct(edge, jnp.float32),
        jax.ShapeDtypeStruct(edge, jnp.float32),
        jax.ShapeDtypeStruct((LZ, slots), jnp.bfloat16),
        jax.ShapeDtypeStruct((SPAN_PAD, slots), jnp.float32),
        jax.ShapeDtypeStruct((SPAN_PAD, slots), jnp.float32),
        jax.ShapeDtypeStruct((side, SPAN_PAD, LZ), jnp.float32),
        jax.ShapeDtypeStruct((side + 1, SPAN_PAD, LZ), jnp.float32),
    ]
    tap_specs = [whole_spec(kernel.shape)] * 2
    return pl.pallas_call(
        spread_kernel,
        grid=(slots // BLOCK,),
        in_specs=[pl.BlockSpec(memory_space=pltpu.SMEM), row, row, weight] + tap_specs,
        out_specs=[whole_spec(part.shape) for part in shapes[:3]]
        + table_specs()
        + [whole_spec(part.shape) for part in shapes[6:]],
        out_shape=shapes,
        scratch_shapes=[
            pltpu.VMEM((FACE, LZ), jnp.float32),
            pltpu.VMEM((SPAN_PAD * SPAN_PAD, LZ), jnp.float32),
        ],
        name="spread",
        compiler_params=pltpu.CompilerParams(vmem_limit_bytes=VMEM_BYTES),
    )(count, charge, cell, weights, kernel, kernel_coarse)


def read_beads(count, grid, tables):
    slots = tables[0].shape[1]
    return pl.pallas_call(
        read_kernel,
        grid=(slots // READ_BLOCK,),
        in_specs=[
            pl.BlockSpec(memory_space=pltpu.SMEM),
            pl.BlockSpec(memory_space=pltpu.VMEM),
        ]
        + table_specs(),
        out_specs=pl.BlockSpec((1, 1, READ_BLOCK), lambda i: (0, 0, i)),
        out_shape=jax.ShapeDtypeStruct((1, 1, slots), jnp.float32),
        name="read",
        compiler_params=pltpu.CompilerParams(vmem_limit_bytes=VMEM_BYTES),
    )(count, grid, *tables)


def spline_of(distance, period):
    place = (distance + 2) & (period - 1)
    return jnp.where(
        place == 2,
        0.75,
        jnp.where(
            (place == 1) | (place == 3), 0.5, jnp.where((place == 0) | (place == 4), 0.125, 0.0)
        ),
    )


PERIOD = 32


def tap_rows(taps):
    side = taps.shape[0]
    tap = lax.broadcasted_iota(jnp.int32, (side, LZ), 0)
    lane = lax.broadcasted_iota(jnp.int32, (side, LZ), 1)
    table = jnp.where(((lane + tap - RADIUS) & (PERIOD - 1)) == 0, 1.0, 0.0).astype(jnp.bfloat16)
    return jnp.dot(taps, table, preferred_element_type=jnp.float32)


def turned(row):
    return pltpu.roll(
        jnp.broadcast_to(row, (PERIOD, row.shape[1])), 0, 1, stride=1, stride_axis=0
    )


def near_mask(rows, depth):
    row = lax.broadcasted_iota(jnp.int32, (rows, LZ), 0)
    lane = lax.broadcasted_iota(jnp.int32, (rows, LZ), 1)
    near = ((row - lane + RADIUS) & (depth - 1)) <= 2 * RADIUS
    return jnp.where(near, 1.0, 0.0).astype(jnp.bfloat16)


def three_terms(value):
    first = value.astype(jnp.bfloat16)
    rest = value - first.astype(jnp.float32)
    second = rest.astype(jnp.bfloat16)
    third = (rest - second.astype(jnp.float32)).astype(jnp.bfloat16)
    return first, second, third


def merged_plane(pieces, plane):
    own, below, above = pieces
    inner = plane - RADIUS
    if inner < 0:
        return below[plane]
    value = own[inner * SPAN_PAD : (inner + 1) * SPAN_PAD] if inner < SPAN else None
    if plane < REACH:
        return value + below[plane]
    if inner < LX:
        return value
    outer = above[inner - LX]
    return outer if value is None else value + outer


def gather_kernel(*refs):
    fine_ref, coarse_ref, up_ref, down_ref, half_ref = refs[-5:]
    own, before = refs[0:3], refs[3:6]
    after = before if len(refs) == 11 else refs[6:9]
    for plane in range(PLANES):
        middle = merged_plane(own, plane)
        lower = merged_plane(before, plane)
        upper = merged_plane(after, plane)
        value = jnp.concatenate(
            [
                lower[8:16],
                middle[0:8] + lower[16:24],
                middle[8:16],
                middle[16:24] + upper[0:8],
                upper[8:24],
            ],
            axis=0,
        )
        fine_ref[plane] = value.astype(jnp.bfloat16).astype(jnp.float32)
    fine_ref[PLANES:] = jnp.zeros_like(fine_ref[PLANES:])
    spline = (0.125, 0.5, 0.75, 0.5, 0.125)
    for plane in range(KNOWN):
        total = spline[0] * fine_ref[2 * plane]
        for step in range(1, 5):
            total = total + spline[step] * fine_ref[2 * plane + step]
        half_ref[plane] = total
    total = spline[0] * half_ref[:, pl.ds(0, KNOWN, stride=2)]
    for step in range(1, 5):
        total = total + spline[step] * half_ref[:, pl.ds(step, KNOWN, stride=2)]
    terms = jnp.concatenate(three_terms(total.reshape(KNOWN * KNOWN, LZ)), axis=1)
    shape = (3 * LZ, LZ)
    fine_depth = lax.broadcasted_iota(jnp.int32, shape, 0) & (LZ - 1)
    coarse_depth = lax.broadcasted_iota(jnp.int32, shape, 1) & (HALF - 1)
    table = spline_of(fine_depth - 2 * coarse_depth, LZ).astype(jnp.bfloat16)
    coarse = jnp.dot(terms, table, preferred_element_type=jnp.float32)
    coarse = coarse.astype(jnp.bfloat16).reshape(coarse_ref.shape)
    coarse_ref[...] = coarse
    up_ref[...] = coarse[2 : 2 + EDGE]
    down_ref[...] = coarse[8 : 8 + EDGE]


def gather_fine(pieces):
    edge = jax.ShapeDtypeStruct((EDGE, KNOWN, LZ), jnp.bfloat16)
    return pl.pallas_call(
        gather_kernel,
        out_shape=(
            jax.ShapeDtypeStruct((PLANES_PAD, COLUMNS, LZ), jnp.float32),
            jax.ShapeDtypeStruct((KNOWN, KNOWN, LZ), jnp.bfloat16),
            edge,
            edge,
        ),
        scratch_shapes=[pltpu.VMEM((KNOWN, COLUMNS, LZ), jnp.float32)],
        name="gather",
        compiler_params=pltpu.CompilerParams(vmem_limit_bytes=VMEM_BYTES),
    )(*pieces)


def fine_kernel(
    fine_ref,
    row_ref,
    coarse_row_ref,
    out_ref,
    coarse_ref,
    pair_ref,
    even_ref,
    odd_ref,
):
    side = row_ref.shape[0]
    flat_ref = fine_ref.reshape(PLANES_PAD * COLUMNS, LZ)
    kept = pair_ref.shape[2] // 8
    for shift in range(SHIFTS):
        halves = [fine_ref[:, pl.ds(2 * shift + part, 8, stride=2)] for part in range(2)]
        both = jnp.concatenate(halves, axis=2)
        for part in range(2):
            pair_ref[part, shift] = (
                both[part : part + kept].reshape(kept * 8, 2 * LZ).astype(jnp.bfloat16)
            )
    out_ref[...] = jnp.zeros_like(out_ref)

    def build(table_ref, plane):
        mask = near_mask(LZ, LZ)
        for band in range(BANDS):
            block = turned(row_ref[plane, band : band + 1]).astype(jnp.bfloat16)
            table_ref[band] = jnp.concatenate([block] * (LZ // PERIOD), axis=0) * mask

    def build_coarse(index, part):
        plane = 2 * index + part
        lower_half = lax.broadcasted_iota(jnp.int32, (PERIOD, LZ), 1) < HALF
        mask = near_mask(HALF, HALF)
        before = turned(coarse_row_ref[plane, 0:1])
        for band in range(BANDS - 1):
            after = turned(coarse_row_ref[plane, band + 1 : band + 2])
            block = jnp.where(lower_half, after, before).astype(jnp.bfloat16)
            start = part * LZ + (band % 2) * HALF
            coarse_ref[index, band // 2, start : start + HALF] = (
                jnp.concatenate([block] * (HALF // PERIOD), axis=0) * mask
            )
            before = after

    def multiply(table_ref, plane, part):
        rows = pl.ds(pl.multiple_of((plane - part) * 8, 16), NEAR)
        far = []
        for pair in range(SHIFTS + 1):
            column = plane * COLUMNS + LY + 2 * pair
            halves = [
                flat_ref[pl.ds(column + half, SPAN_PAD, stride=COLUMNS)] for half in range(2)
            ]
            far.append(jnp.concatenate(halves, axis=1))
        total = out_ref[...]
        for shift in range(SHIFTS):
            band = 2 * shift + 1
            upper = jnp.concatenate([table_ref[band], table_ref[band - 1]], axis=1)
            lower = jnp.concatenate([table_ref[band + 1], table_ref[band]], axis=1)
            outer = jnp.concatenate(far[shift : shift + 2], axis=0).astype(jnp.bfloat16)
            total = total + jnp.dot(
                jnp.concatenate([pair_ref[part, shift, rows], outer], axis=0),
                jnp.concatenate([upper, lower], axis=0),
                preferred_element_type=jnp.float32,
            )
        out_ref[...] = total

    build(even_ref, 0)

    def two_planes(index, carry):
        plane = 2 * index
        build(odd_ref, plane + 1)
        build_coarse(index, 0)
        multiply(even_ref, plane, 0)
        build(even_ref, plane + 2)
        build_coarse(index, 1)
        multiply(odd_ref, plane + 1, 1)
        return carry

    lax.fori_loop(0, side // 2, two_planes, 0)
    build_coarse(side // 2, 0)
    build_coarse(side // 2, 1)
    multiply(even_ref, side - 1, 0)


def fine_sums(fine, rows, rows_coarse):
    side = rows.shape[0]
    pairs = (side + 1) // 2
    return pl.pallas_call(
        fine_kernel,
        out_shape=(
            jax.ShapeDtypeStruct((NEAR + FAR, 2 * LZ), jnp.float32),
            jax.ShapeDtypeStruct((pairs, SHIFTS, 2 * LZ, LZ), jnp.bfloat16),
        ),
        scratch_shapes=[
            pltpu.VMEM((2, SHIFTS, NEAR + 16 * RADIUS, 2 * LZ), jnp.bfloat16),
            pltpu.VMEM((BANDS, LZ, LZ), jnp.bfloat16),
            pltpu.VMEM((BANDS, LZ, LZ), jnp.bfloat16),
        ],
        name="fine",
        compiler_params=pltpu.CompilerParams(vmem_limit_bytes=VMEM_BYTES),
    )(fine, rows, rows_coarse)


def coarse_kernel(
    own_ref,
    below_ref,
    above_ref,
    low_ref,
    high_ref,
    table_ref,
    sums_ref,
    grid_ref,
    face_ref,
    cell_ref,
    pair_ref,
    coarse_ref,
    wide_ref,
    join_ref,
):
    def prepare():
        cell_ref[...] = jnp.zeros_like(cell_ref)
        for start, part in ((0, below_ref), (EDGE, own_ref), (EDGE + KNOWN, above_ref)):
            planes = slice(start, start + part.shape[0])
            values = part[...].astype(jnp.float32)
            cell_ref[planes, 8:24] = values
            if low_ref is None:
                cell_ref[planes, 0:8] = values[:, 8:16]
                cell_ref[planes, 24:32] = values[:, 0:8]
            else:
                cell_ref[planes, 0:8] = low_ref[planes].astype(jnp.float32)
                cell_ref[planes, 24:32] = high_ref[planes].astype(jnp.float32)
        lower_half = lax.broadcasted_iota(jnp.int32, (COARSE_IN + 1, 8, LZ), 2) < HALF
        for shift in range(SHIFTS):
            pair = jnp.where(
                lower_half,
                cell_ref[:, pl.ds(2 * shift + 2, 8, stride=2)],
                cell_ref[:, pl.ds(2 * shift + 3, 8, stride=2)],
            )
            rows = COARSE_IN * 8
            pair_ref[shift] = jnp.concatenate(
                [pair[:COARSE_IN].reshape(rows, LZ), pair[1:].reshape(rows, LZ)], axis=1
            ).astype(jnp.bfloat16)

    prepare()
    total = None
    for pair in range(table_ref.shape[0]):
        rows = slice(pair * 16, pair * 16 + COARSE_OUT * 8)
        for shift in range(SHIFTS):
            part = jnp.dot(
                pair_ref[shift, rows], table_ref[pair, shift], preferred_element_type=jnp.float32
            )
            total = part if total is None else total + part

    def finish():
        high = total.astype(jnp.bfloat16)
        low = (total - high.astype(jnp.float32)).astype(jnp.bfloat16)
        shape = (2 * LZ, 2 * LZ)
        source = lax.broadcasted_iota(jnp.int32, shape, 0)
        target = lax.broadcasted_iota(jnp.int32, shape, 1)
        table = jnp.where(
            (source // HALF) % 2 == target // LZ,
            spline_of((target & (LZ - 1)) - 2 * (source & (HALF - 1)), LZ),
            0.0,
        ).astype(jnp.bfloat16)
        deep = jnp.dot(
            jnp.concatenate([high, low], axis=1), table, preferred_element_type=jnp.float32
        )
        for part in range(2):
            coarse_ref[:, pl.ds(part, 8, stride=2)] = deep[:, part * LZ : (part + 1) * LZ].reshape(
                COARSE_OUT, 8, LZ
            )
        wide_ref[...] = jnp.zeros_like(wide_ref)
        for plane in range(SPAN):
            middle = plane // 2 + 1
            if plane % 2:
                value = (coarse_ref[middle] + coarse_ref[middle + 1]) * 0.5
            else:
                value = (
                    coarse_ref[middle - 1] + 6.0 * coarse_ref[middle] + coarse_ref[middle + 1]
                ) * 0.125
            wide_ref[plane, 0:16] = value
        before = wide_ref[:, 0:16]
        middle = wide_ref[:, 1:17]
        after = wide_ref[:, 2:18]
        even = (before + 6.0 * middle + after) * 0.125
        odd = (middle + after) * 0.5
        near = sums_ref[:NEAR].reshape(SPAN + 1, 8, 2 * LZ)
        join_ref[...] = jnp.zeros_like(join_ref)
        for plane in range(SPAN):
            start = plane * 32
            for part, refined in ((0, even[plane]), (1, odd[plane])):
                join_ref[pl.ds(start + part, 8, stride=2)] = (
                    near[plane, :, part * LZ : (part + 1) * LZ] + refined[:8]
                )
                join_ref[pl.ds(start + 16 + part, 8, stride=2)] = refined[8:]
        for column in range(LY, SPAN):
            pair, part = divmod(column - LY, 2)
            rows = slice(NEAR + pair * SPAN_PAD, NEAR + (pair + 1) * SPAN_PAD)
            join_ref[pl.ds(column, SPAN_PAD, stride=32)] += sums_ref[
                rows, part * LZ : (part + 1) * LZ
            ]
        for plane in range(LX):
            grid_ref[plane] = join_ref[plane * 32 : plane * 32 + LY]
        inside = [join_ref[plane * 32 : plane * 32 + LY] for plane in range(SPAN)]
        outside = [join_ref[pl.ds(column, SPAN_PAD, stride=32)] for column in range(LY, SPAN)]
        face = jnp.concatenate(inside + outside, axis=0)
        face_high = face.astype(jnp.bfloat16)
        face_low = (face - face_high.astype(jnp.float32)).astype(jnp.bfloat16)
        face_ref[:, :LZ] = face_high
        face_ref[:, LZ:] = face_low

    finish()


def potentials(own, below, above, low, high, table, sums):
    given = [own, below, above] + ([] if low is None else [low, high])
    specs = [pl.BlockSpec(memory_space=pltpu.VMEM)] * (len(given) + 2)

    def body(*refs):
        if low is None:
            refs = refs[:3] + (None, None) + refs[3:]
        coarse_kernel(*refs)

    return pl.pallas_call(
        body,
        in_specs=specs,
        out_shape=(
            jax.ShapeDtypeStruct((LX, LY, LZ), jnp.float32),
            jax.ShapeDtypeStruct((FACE, 2 * LZ), jnp.bfloat16),
        ),
        scratch_shapes=[
            pltpu.VMEM((COARSE_IN + 1, 40, LZ), jnp.float32),
            pltpu.VMEM((SHIFTS, COARSE_IN * 8, 2 * LZ), jnp.bfloat16),
            pltpu.VMEM((COARSE_OUT, 16, LZ), jnp.float32),
            pltpu.VMEM((SPAN, 24, LZ), jnp.float32),
            pltpu.VMEM((SPAN_PAD * 32, LZ), jnp.float32),
        ],
        name="coarse",
        compiler_params=pltpu.CompilerParams(vmem_limit_bytes=VMEM_BYTES),
    )(*given, table, sums)


def on_device(bead_charge, bead_cell, bead_count, interp_weights, kernel_fine, kernel_coarse):
    beads = [
        pltpu.with_memory_space_constraint(value, pltpu.HBM)
        for value in (bead_charge, bead_cell, interp_weights, kernel_fine, kernel_coarse)
    ]
    own, up, down, *tables, rows, rows_coarse = spread_beads(bead_count, *beads)
    below = from_behind(up, "gx", 1)
    above = from_behind(down, "gx", -1)
    wraps = lax.axis_size("gy") == 2
    pieces = [own, below, above]
    for steps in (1,) if wraps else (1, -1):
        pieces += [from_behind(part, "gy", steps) for part in (own, below, above)]
    fine, coarse, coarse_up, coarse_down = gather_fine(pieces)
    coarse_below = from_behind(coarse_up, "gx", 1)
    coarse_above = from_behind(coarse_down, "gx", -1)
    sums, table_coarse = fine_sums(fine, rows, rows_coarse)
    low = high = None
    if not wraps:
        joined = jnp.concatenate([coarse_below, coarse, coarse_above], axis=0)
        low = from_behind(joined[:, :8], "gy", 1)
        high = from_behind(joined[:, 8:], "gy", -1)
    potential_grid, face = potentials(
        coarse, coarse_below, coarse_above, low, high, table_coarse, sums
    )
    bead_potential = read_beads(bead_count, face, tables)
    return (bead_potential, potential_grid)


def solution(mesh):
    return jax.shard_map(
        on_device,
        mesh=mesh,
        in_specs=(
            P("gx", "gy", None),
            P("gx", "gy", None),
            P("gx", "gy"),
            P("gx", "gy", None, None),
            P(),
            P(),
        ),
        out_specs=(P("gx", "gy", None), P("gx", "gy", None)),
        check_vma=False,
    )
```

```python
import jax
import jax.numpy as jnp
from jax import lax
from jax.experimental import pallas as pl
from jax.experimental.pallas import tpu as pltpu
from jax.sharding import PartitionSpec as P

LX = 16
LY = 16
LZ = 128
RADIUS = 8

SPAN = LX + 3
SPAN_PAD = 24
BLOCK = 8192
CHUNK = 256
READ_CHUNK = 512
READ_BLOCK = 8192
FACE = SPAN * LY + (SPAN - LY) * SPAN_PAD
VMEM_BYTES = 24 * 1024 * 1024
REACH = 11
PLANES = SPAN + 2 * RADIUS
PLANES_PAD = 40
COLUMNS = 48
NEAR = (SPAN + 1) * 8
FAR = 2 * SPAN_PAD
SHIFTS = RADIUS + 1
BANDS = 2 * RADIUS + 3
HALF = LZ // 2
KNOWN = 16
EDGE = 6
COARSE_OUT = 12
COARSE_IN = COARSE_OUT + 2 * RADIUS


def from_behind(value, axis, steps):
    count = lax.axis_size(axis)
    pairs = [(source, (source + steps) % count) for source in range(count)]
    return lax.ppermute(value, axis, pairs)


def hat_rows(rows, start, weights, period):
    places = lax.broadcasted_iota(jnp.int32, (rows, start.shape[1]), 0) - start
    if period:
        places = places & (period - 1)
    table = jnp.where(places == 3, weights[3:4], 0.0)
    for offset in (2, 1, 0):
        table = jnp.where(places == offset, weights[offset : offset + 1], table)
    return table


def depth_rows(start, weights):
    groups = LZ // 8
    pattern = hat_rows(16, start & 7, weights, 0)
    low, high = pattern[:8], pattern[8:]
    group = jnp.broadcast_to(start // 8, low.shape)
    here = [group == place for place in range(groups)]
    rows = [
        jnp.where(here[place], low, jnp.where(here[place - 1], high, 0.0))
        for place in range(groups)
    ]
    return jnp.concatenate(rows, axis=0)


def bead_tables(cells, weights):
    first = hat_rows(SPAN_PAD, cells // (LY * LZ), weights[0:4], 0)
    second = hat_rows(SPAN_PAD, cells // LZ % LY, weights[4:8], 0)
    depth = depth_rows(cells % LZ, weights[8:12])
    return first, second, depth


def face_rows(first, second):
    inside = [first[row : row + 1] * second[:LY] for row in range(SPAN)]
    outside = [second[row : row + 1] * first for row in range(LY, SPAN)]
    return jnp.concatenate(inside + outside, axis=0)


def spread_kernel(
    count_ref,
    charge_ref,
    cell_ref,
    weight_ref,
    tap_ref,
    coarse_tap_ref,
    out_ref,
    up_ref,
    down_ref,
    depth_ref,
    first_ref,
    second_ref,
    row_ref,
    coarse_row_ref,
    total_ref,
    order_ref,
):
    step = pl.program_id(0)

    @pl.when(step == 0)
    def _():
        total_ref[...] = jnp.zeros_like(total_ref)
        row_ref[...] = jnp.zeros_like(row_ref)
        coarse_row_ref[...] = jnp.zeros_like(coarse_row_ref)
        side = tap_ref.shape[0]
        for plane in range(side):
            row_ref[plane, 1 : 1 + side] = tap_rows(tap_ref[plane])
            coarse_row_ref[plane, 1 : 1 + side] = tap_rows(coarse_tap_ref[plane])

    dims = (((1,), (1,)), ((), ()))
    total = None
    for start in range(0, BLOCK, CHUNK):
        beads = slice(start, start + CHUNK)
        cells = cell_ref[0, :, beads]
        weights = weight_ref[0, 0, :, beads].astype(jnp.float32)
        first, second, depth = bead_tables(cells, weights)
        depth = depth.astype(jnp.bfloat16)
        kept = pl.ds(pl.multiple_of(step * BLOCK, BLOCK) + start, CHUNK)
        depth_ref[:, kept] = depth
        first_ref[:, kept] = first
        second_ref[:, kept] = second
        slots = lax.broadcasted_iota(jnp.int32, cells.shape, 1) + (step * BLOCK + start)
        amount = jnp.where(slots < count_ref[0, 0], charge_ref[0, :, beads], 0.0)
        face = face_rows(first * amount, second)
        high = face.astype(jnp.bfloat16)
        low = (face - high.astype(jnp.float32)).astype(jnp.bfloat16)
        for term in (high, low):
            part = lax.dot_general(term, depth, dims, preferred_element_type=jnp.float32)
            total = part if total is None else total + part
    total_ref[...] += total

    @pl.when(step == pl.num_programs(0) - 1)
    def _():
        order_ref[...] = jnp.zeros_like(order_ref)
        for plane in range(SPAN):
            order_ref[plane * SPAN_PAD : plane * SPAN_PAD + LY] = total_ref[
                plane * LY : (plane + 1) * LY
            ]
        for column in range(SPAN - LY):
            start = SPAN * LY + column * SPAN_PAD
            order_ref[pl.ds(LY + column, SPAN_PAD, stride=SPAN_PAD)] = total_ref[
                start : start + SPAN_PAD
            ]
        out_ref[...] = order_ref[: SPAN * SPAN_PAD]
        up_ref[...] = order_ref[(SPAN - REACH) * SPAN_PAD : SPAN * SPAN_PAD].reshape(up_ref.shape)
        down_ref[...] = order_ref[: REACH * SPAN_PAD].reshape(down_ref.shape)


def read_kernel(count_ref, grid_ref, depth_ref, first_ref, second_ref, out_ref):
    step = pl.program_id(0)
    for start in range(0, READ_BLOCK, READ_CHUNK):
        beads = slice(start, start + READ_CHUNK)
        kept = pl.ds(pl.multiple_of(step * READ_BLOCK, READ_BLOCK) + start, READ_CHUNK)
        depth = depth_ref[:, kept]
        along = jnp.dot(
            grid_ref[...],
            jnp.concatenate([depth, depth], axis=0),
            preferred_element_type=jnp.float32,
        )
        first = first_ref[:, kept]
        second = second_ref[:, kept]
        inside = first[0:1] * along[0:LY]
        for row in range(1, SPAN):
            inside = inside + first[row : row + 1] * along[row * LY : (row + 1) * LY]
        inside = inside * second[:LY]
        outside = None
        for column in range(SPAN - LY):
            place = SPAN * LY + column * SPAN_PAD
            part = second[LY + column : LY + column + 1] * along[place : place + SPAN_PAD]
            outside = part if outside is None else outside + part
        outside = outside * first
        parts = [inside[row : row + 8] for row in range(0, LY, 8)]
        parts += [outside[row : row + 8] for row in range(0, SPAN_PAD, 8)]
        picked = jnp.sum(sum(parts[1:], parts[0]), axis=0, keepdims=True)
        slots = lax.broadcasted_iota(jnp.int32, picked.shape, 1) + (step * READ_BLOCK + start)
        out_ref[0, :, beads] = jnp.where(slots < count_ref[0, 0], picked, 0.0)


def whole_spec(shape):
    return pl.BlockSpec(shape, lambda i: (0,) * len(shape))


def table_specs():
    return [pl.BlockSpec(memory_space=pltpu.VMEM)] * 3


def spread_beads(count, charge, cell, weights, kernel, kernel_coarse):
    slots = charge.shape[2]
    row = pl.BlockSpec((1, 1, BLOCK), lambda i: (0, 0, i))
    weight = pl.BlockSpec((1, 1, 12, BLOCK), lambda i: (0, 0, 0, i))
    edge = (REACH, SPAN_PAD, LZ)
    side = kernel.shape[0]
    shapes = [
        jax.ShapeDtypeStruct((SPAN * SPAN_PAD, LZ), jnp.float32),
        jax.ShapeDtypeStruct(edge, jnp.float32),
        jax.ShapeDtypeStruct(edge, jnp.float32),
        jax.ShapeDtypeStruct((LZ, slots), jnp.bfloat16),
        jax.ShapeDtypeStruct((SPAN_PAD, slots), jnp.float32),
        jax.ShapeDtypeStruct((SPAN_PAD, slots), jnp.float32),
        jax.ShapeDtypeStruct((side, SPAN_PAD, LZ), jnp.float32),
        jax.ShapeDtypeStruct((side + 1, SPAN_PAD, LZ), jnp.float32),
    ]
    tap_specs = [whole_spec(kernel.shape)] * 2
    return pl.pallas_call(
        spread_kernel,
        grid=(slots // BLOCK,),
        in_specs=[pl.BlockSpec(memory_space=pltpu.SMEM), row, row, weight] + tap_specs,
        out_specs=[whole_spec(part.shape) for part in shapes[:3]]
        + table_specs()
        + [whole_spec(part.shape) for part in shapes[6:]],
        out_shape=shapes,
        scratch_shapes=[
            pltpu.VMEM((FACE, LZ), jnp.float32),
            pltpu.VMEM((SPAN_PAD * SPAN_PAD, LZ), jnp.float32),
        ],
        name="spread",
        compiler_params=pltpu.CompilerParams(vmem_limit_bytes=VMEM_BYTES),
    )(count, charge, cell, weights, kernel, kernel_coarse)


def read_beads(count, grid, tables):
    slots = tables[0].shape[1]
    return pl.pallas_call(
        read_kernel,
        grid=(slots // READ_BLOCK,),
        in_specs=[
            pl.BlockSpec(memory_space=pltpu.SMEM),
            pl.BlockSpec(memory_space=pltpu.VMEM),
        ]
        + table_specs(),
        out_specs=pl.BlockSpec((1, 1, READ_BLOCK), lambda i: (0, 0, i)),
        out_shape=jax.ShapeDtypeStruct((1, 1, slots), jnp.float32),
        name="read",
        compiler_params=pltpu.CompilerParams(vmem_limit_bytes=VMEM_BYTES),
    )(count, grid, *tables)


def spline_of(distance, period):
    place = (distance + 2) & (period - 1)
    return jnp.where(
        place == 2,
        0.75,
        jnp.where(
            (place == 1) | (place == 3), 0.5, jnp.where((place == 0) | (place == 4), 0.125, 0.0)
        ),
    )


PERIOD = 32


def tap_rows(taps):
    side = taps.shape[0]
    tap = lax.broadcasted_iota(jnp.int32, (side, LZ), 0)
    lane = lax.broadcasted_iota(jnp.int32, (side, LZ), 1)
    table = jnp.where(((lane + tap - RADIUS) & (PERIOD - 1)) == 0, 1.0, 0.0).astype(jnp.bfloat16)
    return jnp.dot(taps, table, preferred_element_type=jnp.float32)


def turned(row):
    return pltpu.roll(
        jnp.broadcast_to(row, (PERIOD, row.shape[1])), 0, 1, stride=1, stride_axis=0
    )


def near_mask(rows, depth):
    row = lax.broadcasted_iota(jnp.int32, (rows, LZ), 0)
    lane = lax.broadcasted_iota(jnp.int32, (rows, LZ), 1)
    near = ((row - lane + RADIUS) & (depth - 1)) <= 2 * RADIUS
    return jnp.where(near, 1.0, 0.0).astype(jnp.bfloat16)


def three_terms(value):
    first = value.astype(jnp.bfloat16)
    rest = value - first.astype(jnp.float32)
    second = rest.astype(jnp.bfloat16)
    third = (rest - second.astype(jnp.float32)).astype(jnp.bfloat16)
    return first, second, third


def merged_plane(pieces, plane):
    own, below, above = pieces
    inner = plane - RADIUS
    if inner < 0:
        return below[plane]
    value = own[inner * SPAN_PAD : (inner + 1) * SPAN_PAD] if inner < SPAN else None
    if plane < REACH:
        return value + below[plane]
    if inner < LX:
        return value
    outer = above[inner - LX]
    return outer if value is None else value + outer


def gather_kernel(*refs):
    fine_ref, coarse_ref, up_ref, down_ref, half_ref = refs[-5:]
    own, before = refs[0:3], refs[3:6]
    after = before if len(refs) == 11 else refs[6:9]
    for plane in range(PLANES):
        middle = merged_plane(own, plane)
        lower = merged_plane(before, plane)
        upper = merged_plane(after, plane)
        value = jnp.concatenate(
            [
                lower[8:16],
                middle[0:8] + lower[16:24],
                middle[8:16],
                middle[16:24] + upper[0:8],
                upper[8:24],
            ],
            axis=0,
        )
        fine_ref[plane] = value.astype(jnp.bfloat16).astype(jnp.float32)
    fine_ref[PLANES:] = jnp.zeros_like(fine_ref[PLANES:])
    spline = (0.125, 0.5, 0.75, 0.5, 0.125)
    for plane in range(KNOWN):
        total = spline[0] * fine_ref[2 * plane]
        for step in range(1, 5):
            total = total + spline[step] * fine_ref[2 * plane + step]
        half_ref[plane] = total
    total = spline[0] * half_ref[:, pl.ds(0, KNOWN, stride=2)]
    for step in range(1, 5):
        total = total + spline[step] * half_ref[:, pl.ds(step, KNOWN, stride=2)]
    terms = jnp.concatenate(three_terms(total.reshape(KNOWN * KNOWN, LZ)), axis=1)
    shape = (3 * LZ, LZ)
    fine_depth = lax.broadcasted_iota(jnp.int32, shape, 0) & (LZ - 1)
    coarse_depth = lax.broadcasted_iota(jnp.int32, shape, 1) & (HALF - 1)
    table = spline_of(fine_depth - 2 * coarse_depth, LZ).astype(jnp.bfloat16)
    coarse = jnp.dot(terms, table, preferred_element_type=jnp.float32)
    coarse = coarse.astype(jnp.bfloat16).reshape(coarse_ref.shape)
    coarse_ref[...] = coarse
    up_ref[...] = coarse[2 : 2 + EDGE]
    down_ref[...] = coarse[8 : 8 + EDGE]


def gather_fine(pieces):
    edge = jax.ShapeDtypeStruct((EDGE, KNOWN, LZ), jnp.bfloat16)
    return pl.pallas_call(
        gather_kernel,
        out_shape=(
            jax.ShapeDtypeStruct((PLANES_PAD, COLUMNS, LZ), jnp.float32),
            jax.ShapeDtypeStruct((KNOWN, KNOWN, LZ), jnp.bfloat16),
            edge,
            edge,
        ),
        scratch_shapes=[pltpu.VMEM((KNOWN, COLUMNS, LZ), jnp.float32)],
        name="gather",
        compiler_params=pltpu.CompilerParams(vmem_limit_bytes=VMEM_BYTES),
    )(*pieces)


def fine_kernel(
    fine_ref,
    row_ref,
    coarse_row_ref,
    out_ref,
    coarse_ref,
    pair_ref,
    even_ref,
    odd_ref,
):
    side = row_ref.shape[0]
    flat_ref = fine_ref.reshape(PLANES_PAD * COLUMNS, LZ)
    kept = pair_ref.shape[2] // 8
    for shift in range(SHIFTS):
        halves = [fine_ref[:, pl.ds(2 * shift + part, 8, stride=2)] for part in range(2)]
        both = jnp.concatenate(halves, axis=2)
        for part in range(2):
            pair_ref[part, shift] = (
                both[part : part + kept].reshape(kept * 8, 2 * LZ).astype(jnp.bfloat16)
            )
    out_ref[...] = jnp.zeros_like(out_ref)

    def build(table_ref, plane):
        mask = near_mask(LZ, LZ)
        for band in range(BANDS):
            block = turned(row_ref[plane, band : band + 1]).astype(jnp.bfloat16)
            table_ref[band] = jnp.concatenate([block] * (LZ // PERIOD), axis=0) * mask

    def build_coarse(index, part):
        plane = 2 * index + part
        lower_half = lax.broadcasted_iota(jnp.int32, (PERIOD, LZ), 1) < HALF
        mask = near_mask(HALF, HALF)
        before = turned(coarse_row_ref[plane, 0:1])
        for band in range(BANDS - 1):
            after = turned(coarse_row_ref[plane, band + 1 : band + 2])
            block = jnp.where(lower_half, after, before).astype(jnp.bfloat16)
            start = part * LZ + (band % 2) * HALF
            coarse_ref[index, band // 2, start : start + HALF] = (
                jnp.concatenate([block] * (HALF // PERIOD), axis=0) * mask
            )
            before = after

    def multiply(table_ref, plane, part):
        rows = pl.ds(pl.multiple_of((plane - part) * 8, 16), NEAR)
        far = []
        for pair in range(SHIFTS + 1):
            column = plane * COLUMNS + LY + 2 * pair
            halves = [
                flat_ref[pl.ds(column + half, SPAN_PAD, stride=COLUMNS)] for half in range(2)
            ]
            far.append(jnp.concatenate(halves, axis=1))
        total = out_ref[...]
        for shift in range(SHIFTS):
            band = 2 * shift + 1
            upper = jnp.concatenate([table_ref[band], table_ref[band - 1]], axis=1)
            lower = jnp.concatenate([table_ref[band + 1], table_ref[band]], axis=1)
            outer = jnp.concatenate(far[shift : shift + 2], axis=0).astype(jnp.bfloat16)
            total = total + jnp.dot(
                jnp.concatenate([pair_ref[part, shift, rows], outer], axis=0),
                jnp.concatenate([upper, lower], axis=0),
                preferred_element_type=jnp.float32,
            )
        out_ref[...] = total

    build(even_ref, 0)

    def two_planes(index, carry):
        plane = 2 * index
        build(odd_ref, plane + 1)
        build_coarse(index, 0)
        multiply(even_ref, plane, 0)
        build(even_ref, plane + 2)
        build_coarse(index, 1)
        multiply(odd_ref, plane + 1, 1)
        return carry

    lax.fori_loop(0, side // 2, two_planes, 0)
    build_coarse(side // 2, 0)
    build_coarse(side // 2, 1)
    multiply(even_ref, side - 1, 0)


def fine_sums(fine, rows, rows_coarse):
    side = rows.shape[0]
    pairs = (side + 1) // 2
    return pl.pallas_call(
        fine_kernel,
        out_shape=(
            jax.ShapeDtypeStruct((NEAR + FAR, 2 * LZ), jnp.float32),
            jax.ShapeDtypeStruct((pairs, SHIFTS, 2 * LZ, LZ), jnp.bfloat16),
        ),
        scratch_shapes=[
            pltpu.VMEM((2, SHIFTS, NEAR + 16 * RADIUS, 2 * LZ), jnp.bfloat16),
            pltpu.VMEM((BANDS, LZ, LZ), jnp.bfloat16),
            pltpu.VMEM((BANDS, LZ, LZ), jnp.bfloat16),
        ],
        name="fine",
        compiler_params=pltpu.CompilerParams(vmem_limit_bytes=VMEM_BYTES),
    )(fine, rows, rows_coarse)


def coarse_kernel(
    own_ref,
    below_ref,
    above_ref,
    low_ref,
    high_ref,
    table_ref,
    sums_ref,
    grid_ref,
    face_ref,
    cell_ref,
    pair_ref,
    coarse_ref,
    wide_ref,
    join_ref,
):
    def prepare():
        cell_ref[...] = jnp.zeros_like(cell_ref)
        for start, part in ((0, below_ref), (EDGE, own_ref), (EDGE + KNOWN, above_ref)):
            planes = slice(start, start + part.shape[0])
            values = part[...].astype(jnp.float32)
            cell_ref[planes, 8:24] = values
            if low_ref is None:
                cell_ref[planes, 0:8] = values[:, 8:16]
                cell_ref[planes, 24:32] = values[:, 0:8]
            else:
                cell_ref[planes, 0:8] = low_ref[planes].astype(jnp.float32)
                cell_ref[planes, 24:32] = high_ref[planes].astype(jnp.float32)
        lower_half = lax.broadcasted_iota(jnp.int32, (COARSE_IN + 1, 8, LZ), 2) < HALF
        for shift in range(SHIFTS):
            pair = jnp.where(
                lower_half,
                cell_ref[:, pl.ds(2 * shift + 2, 8, stride=2)],
                cell_ref[:, pl.ds(2 * shift + 3, 8, stride=2)],
            )
            rows = COARSE_IN * 8
            pair_ref[shift] = jnp.concatenate(
                [pair[:COARSE_IN].reshape(rows, LZ), pair[1:].reshape(rows, LZ)], axis=1
            ).astype(jnp.bfloat16)

    prepare()
    total = None
    for pair in range(table_ref.shape[0]):
        rows = slice(pair * 16, pair * 16 + COARSE_OUT * 8)
        for shift in range(SHIFTS):
            part = jnp.dot(
                pair_ref[shift, rows], table_ref[pair, shift], preferred_element_type=jnp.float32
            )
            total = part if total is None else total + part

    def finish():
        high = total.astype(jnp.bfloat16)
        low = (total - high.astype(jnp.float32)).astype(jnp.bfloat16)
        shape = (2 * LZ, 2 * LZ)
        source = lax.broadcasted_iota(jnp.int32, shape, 0)
        target = lax.broadcasted_iota(jnp.int32, shape, 1)
        table = jnp.where(
            (source // HALF) % 2 == target // LZ,
            spline_of((target & (LZ - 1)) - 2 * (source & (HALF - 1)), LZ),
            0.0,
        ).astype(jnp.bfloat16)
        deep = jnp.dot(
            jnp.concatenate([high, low], axis=1), table, preferred_element_type=jnp.float32
        )
        for part in range(2):
            coarse_ref[:, pl.ds(part, 8, stride=2)] = deep[:, part * LZ : (part + 1) * LZ].reshape(
                COARSE_OUT, 8, LZ
            )
        wide_ref[...] = jnp.zeros_like(wide_ref)
        for plane in range(SPAN):
            middle = plane // 2 + 1
            if plane % 2:
                value = (coarse_ref[middle] + coarse_ref[middle + 1]) * 0.5
            else:
                value = (
                    coarse_ref[middle - 1] + 6.0 * coarse_ref[middle] + coarse_ref[middle + 1]
                ) * 0.125
            wide_ref[plane, 0:16] = value
        before = wide_ref[:, 0:16]
        middle = wide_ref[:, 1:17]
        after = wide_ref[:, 2:18]
        even = (before + 6.0 * middle + after) * 0.125
        odd = (middle + after) * 0.5
        near = sums_ref[:NEAR].reshape(SPAN + 1, 8, 2 * LZ)
        join_ref[...] = jnp.zeros_like(join_ref)
        for plane in range(SPAN):
            start = plane * 32
            for part, refined in ((0, even[plane]), (1, odd[plane])):
                join_ref[pl.ds(start + part, 8, stride=2)] = (
                    near[plane, :, part * LZ : (part + 1) * LZ] + refined[:8]
                )
                join_ref[pl.ds(start + 16 + part, 8, stride=2)] = refined[8:]
        for column in range(LY, SPAN):
            pair, part = divmod(column - LY, 2)
            rows = slice(NEAR + pair * SPAN_PAD, NEAR + (pair + 1) * SPAN_PAD)
            join_ref[pl.ds(column, SPAN_PAD, stride=32)] += sums_ref[
                rows, part * LZ : (part + 1) * LZ
            ]
        for plane in range(LX):
            grid_ref[plane] = join_ref[plane * 32 : plane * 32 + LY]
        inside = [join_ref[plane * 32 : plane * 32 + LY] for plane in range(SPAN)]
        outside = [join_ref[pl.ds(column, SPAN_PAD, stride=32)] for column in range(LY, SPAN)]
        face = jnp.concatenate(inside + outside, axis=0)
        face_high = face.astype(jnp.bfloat16)
        face_low = (face - face_high.astype(jnp.float32)).astype(jnp.bfloat16)
        face_ref[:, :LZ] = face_high
        face_ref[:, LZ:] = face_low

    finish()


def potentials(own, below, above, low, high, table, sums):
    given = [own, below, above] + ([] if low is None else [low, high])
    specs = [pl.BlockSpec(memory_space=pltpu.VMEM)] * (len(given) + 2)

    def body(*refs):
        if low is None:
            refs = refs[:3] + (None, None) + refs[3:]
        coarse_kernel(*refs)

    return pl.pallas_call(
        body,
        in_specs=specs,
        out_shape=(
            jax.ShapeDtypeStruct((LX, LY, LZ), jnp.float32),
            jax.ShapeDtypeStruct((FACE, 2 * LZ), jnp.bfloat16),
        ),
        scratch_shapes=[
            pltpu.VMEM((COARSE_IN + 1, 40, LZ), jnp.float32),
            pltpu.VMEM((SHIFTS, COARSE_IN * 8, 2 * LZ), jnp.bfloat16),
            pltpu.VMEM((COARSE_OUT, 16, LZ), jnp.float32),
            pltpu.VMEM((SPAN, 24, LZ), jnp.float32),
            pltpu.VMEM((SPAN_PAD * 32, LZ), jnp.float32),
        ],
        name="coarse",
        compiler_params=pltpu.CompilerParams(vmem_limit_bytes=VMEM_BYTES),
    )(*given, table, sums)


def on_device(bead_charge, bead_cell, bead_count, interp_weights, kernel_fine, kernel_coarse):
    beads = [
        pltpu.with_memory_space_constraint(value, pltpu.HBM)
        for value in (bead_charge, bead_cell, interp_weights, kernel_fine, kernel_coarse)
    ]
    own, up, down, *tables, rows, rows_coarse = spread_beads(bead_count, *beads)
    below = from_behind(up, "gx", 1)
    above = from_behind(down, "gx", -1)
    wraps = lax.axis_size("gy") == 2
    pieces = [own, below, above]
    for steps in (1,) if wraps else (1, -1):
        pieces += [from_behind(part, "gy", steps) for part in (own, below, above)]
    fine, coarse, coarse_up, coarse_down = gather_fine(pieces)
    coarse_below = from_behind(coarse_up, "gx", 1)
    coarse_above = from_behind(coarse_down, "gx", -1)
    sums, table_coarse = fine_sums(fine, rows, rows_coarse)
    low = high = None
    if not wraps:
        joined = jnp.concatenate([coarse_below, coarse, coarse_above], axis=0)
        low = from_behind(joined[:, :8], "gy", 1)
        high = from_behind(joined[:, 8:], "gy", -1)
    potential_grid, face = potentials(
        coarse, coarse_below, coarse_above, low, high, table_coarse, sums
    )
    bead_potential = read_beads(bead_count, face, tables)
    return (bead_potential, potential_grid)


def solution(mesh):
    return jax.shard_map(
        on_device,
        mesh=mesh,
        in_specs=(
            P("gx", "gy", None),
            P("gx", "gy", None),
            P("gx", "gy"),
            P("gx", "gy", None, None),
            P(),
            P(),
        ),
        out_specs=(P("gx", "gy", None), P("gx", "gy", None)),
        check_vma=False,
    )
```
